128 devices in a mesh: dp: 1, ep: 128 (over z, y, x, core).
Axes of the slice: x: 4, y: 4, z: 4, core: 2. Of those that a mesh axis runs over, the one named last changes fastest.
Arguments:
- tokens: bfloat16 [8192, 2048], P(('dp', 'ep'))
- expert_ids: int32 [8192, 8], P(('dp', 'ep'))
- gate_w: float32 [8192, 8], P(('dp', 'ep'))
- route_counts: int32 [128, 128], P(('dp', 'ep'))
- w_gate: bfloat16 [128, 2048, 768], P('ep')
- w_up: bfloat16 [128, 2048, 768], P('ep')
- w_down: bfloat16 [128, 768, 2048], P('ep')
Outputs:
- output: bfloat16 [8192, 2048], P(('dp', 'ep'))
All inputs are finite; a program needn't handle non-finite values.
Results may differ from the reference program's by a relative error of at most 0.00369945.
Values are sent between devices in bfloat16 or wider.
A program may use at most 1 GiB of HBM per device.

```python
import jax
import jax.numpy as jnp
from jax import lax

GROUP_SIZE = 128
TOKENS_DEV = 64
MODEL_DIM = 2048
FFN_DIM = 768
NUM_EXPERTS = 128
TOP_K = 8
CAPACITY = 32
HOT_DEVS = 16

LOCAL_EXPERTS = NUM_EXPERTS // GROUP_SIZE
GROUP_ROWS = GROUP_SIZE * TOKENS_DEV


def draw_routing(route_key):
    key_hot, key_star, key_noise, key_cover = jax.random.split(route_key, 4)
    expert_ar = jnp.arange(NUM_EXPERTS)
    expert_dev = expert_ar // LOCAL_EXPERTS
    hot_base = jax.random.randint(key_hot, (), 0, GROUP_SIZE)
    hot_list = (hot_base + jnp.arange(HOT_DEVS) * (GROUP_SIZE // HOT_DEVS)) % GROUP_SIZE
    is_hot = jnp.any(expert_dev[:, None] == hot_list[None, :], axis=1)
    star_expert = hot_base * LOCAL_EXPERTS + jax.random.randint(key_star, (), 0, LOCAL_EXPERTS)
    bonus_int = jnp.where(is_hot, 50, 0) + jnp.where(expert_ar == star_expert, 1000, 0)
    noise_int = jax.random.randint(key_noise, (GROUP_SIZE, TOKENS_DEV, NUM_EXPERTS), 0, 100)
    source = jnp.arange(GROUP_SIZE)
    tok_ar = jnp.arange(TOKENS_DEV)
    choice = jnp.arange(TOP_K)
    cover_rank = tok_ar[:, None] * (TOP_K - 1) + choice[None, :] - 1
    forced = (choice[None, :] >= 1) & (cover_rank < GROUP_SIZE - 1)
    cover_dev = (source[:, None, None] + 1 + cover_rank[None, :, :]) % GROUP_SIZE
    cover_exp = cover_dev * LOCAL_EXPERTS + jax.random.randint(key_cover, (GROUP_SIZE, TOKENS_DEV, TOP_K), 0, LOCAL_EXPERTS)
    taken_mask = jnp.any((cover_exp[:, :, :, None] == expert_ar) & forced[None, :, :, None], axis=2)
    home_mask = (expert_dev[None, :] == source[:, None])[:, None, :]
    pick_score = jnp.where(home_mask | taken_mask, -1, noise_int + bonus_int[None, None, :])
    ranked = lax.top_k(pick_score * NUM_EXPERTS + expert_ar, TOP_K)[1]
    n_forced = jnp.sum(forced.astype(jnp.int32), axis=1)
    pick_col = jnp.clip(jnp.where(choice[None, :] == 0, 0, choice[None, :] - n_forced[:, None]), 0, TOP_K - 1)
    free_exp = jnp.take_along_axis(ranked, jnp.broadcast_to(pick_col[None, :, :], ranked.shape), axis=2)
    expert_ids = jnp.where(forced[None, :, :], cover_exp, free_exp).astype(jnp.int32)
    onehot = (expert_ids.reshape(GROUP_SIZE, TOKENS_DEV * TOP_K, 1) == expert_ar).astype(jnp.int32)
    route_counts = jnp.minimum(jnp.sum(onehot, axis=1), CAPACITY).astype(jnp.int32)
    return expert_ids.reshape(GROUP_ROWS, TOP_K), route_counts


def setup_inputs(seed: int = 0, part: int = 0) -> dict:
    base_key = jax.random.key(seed)
    part_key = jax.random.fold_in(base_key, part)
    key_route, key_tok, key_gate = jax.random.split(part_key, 3)
    key_wg, key_wu, key_wd = jax.random.split(jax.random.key(seed + 1), 3)
    expert_ids, route_counts = draw_routing(key_route)
    tokens = jax.random.normal(key_tok, (GROUP_ROWS, MODEL_DIM), jnp.float32).astype(jnp.bfloat16)
    gate_w = jax.nn.softmax(jax.random.normal(key_gate, (GROUP_ROWS, TOP_K), jnp.float32), axis=-1)
    w_gate = (jax.random.normal(key_wg, (NUM_EXPERTS, MODEL_DIM, FFN_DIM), jnp.float32) * MODEL_DIM ** -0.5).astype(jnp.bfloat16)
    w_up = (jax.random.normal(key_wu, (NUM_EXPERTS, MODEL_DIM, FFN_DIM), jnp.float32) * MODEL_DIM ** -0.5).astype(jnp.bfloat16)
    w_down = (jax.random.normal(key_wd, (NUM_EXPERTS, FFN_DIM, MODEL_DIM), jnp.float32) * FFN_DIM ** -0.5).astype(jnp.bfloat16)
    return {"tokens": tokens, "expert_ids": expert_ids, "gate_w": gate_w, "route_counts": route_counts, "w_gate": w_gate, "w_up": w_up, "w_down": w_down}


def reference(tokens, expert_ids, gate_w, route_counts, w_gate, w_up, w_down):
    expert_ar = jnp.arange(NUM_EXPERTS)
    flat_ids = expert_ids.reshape(GROUP_SIZE, TOKENS_DEV * TOP_K)
    onehot = (flat_ids[:, :, None] == expert_ar).astype(jnp.int32)
    before = jnp.cumsum(onehot, axis=1) - onehot
    slot_idx = jnp.sum(before * onehot, axis=2).reshape(GROUP_SIZE, TOKENS_DEV, TOP_K)
    row_limit = jnp.sum(onehot * route_counts[:, None, :], axis=2).reshape(GROUP_SIZE, TOKENS_DEV, TOP_K)
    kept_mask = slot_idx < row_limit
    ids_3d = expert_ids.reshape(GROUP_SIZE, TOKENS_DEV, TOP_K)
    gates_3d = gate_w.reshape(GROUP_SIZE, TOKENS_DEV, TOP_K)
    tok_3d = tokens.reshape(GROUP_SIZE, TOKENS_DEV, MODEL_DIM).astype(jnp.float32)
    slot_hit = slot_idx[:, None, :, :] == jnp.arange(CAPACITY)[None, :, None, None]

    def one_expert(acc_out, blk_args):
        expert_id, gate_mat, up_mat, down_mat = blk_args
        place_mask = slot_hit & ((ids_3d == expert_id) & kept_mask)[:, None, :, :]
        disp_mat = jnp.sum(place_mask.astype(jnp.float32), axis=3)
        comb_w = jnp.sum(jnp.where(place_mask, gates_3d[:, None, :, :], 0.0), axis=3)
        rows_in = jnp.einsum("gct,gtd->gcd", disp_mat, tok_3d).astype(jnp.bfloat16).reshape(GROUP_SIZE * CAPACITY, MODEL_DIM)
        act_a = jnp.dot(rows_in, gate_mat, preferred_element_type=jnp.float32)
        act_b = jnp.dot(rows_in, up_mat, preferred_element_type=jnp.float32)
        hidden = (jax.nn.silu(act_a) * act_b).astype(jnp.bfloat16)
        rows_out = jnp.dot(hidden, down_mat, preferred_element_type=jnp.float32).astype(jnp.bfloat16)
        rows_out = rows_out.reshape(GROUP_SIZE, CAPACITY, MODEL_DIM).astype(jnp.float32)
        return acc_out + jnp.einsum("gct,gcd->gtd", comb_w, rows_out), None

    summed = lax.scan(one_expert, tok_3d, (expert_ar, w_gate, w_up, w_down))[0]
    return summed.astype(jnp.bfloat16).reshape(GROUP_ROWS, MODEL_DIM)
```

```python
import functools

import jax
import jax.numpy as jnp
from jax import lax
from jax.experimental import pallas as pl
from jax.experimental.pallas import tpu as pltpu
from jax.sharding import PartitionSpec as P

MESH = pl.DeviceIdType.MESH
VMEM = pltpu.VMEM
ANY = pl.ANY
GRP = 8
PLN = 16
CAP_C = 32
CAP_R = 48
CH_R, CH_C = 128, 256
K = 72
D = 7
T = K + 3 * D
N_RING = K + 2 * D
N_SEM = 32
INJ = 12


def place_rows(expert_ids, counts_row, cap_rows, n_exp):
    tok_n, top_n = expert_ids.shape
    flat_ids = expert_ids.reshape(tok_n * top_n)
    onehot = (flat_ids[:, None] == jnp.arange(n_exp)[None, :]).astype(jnp.int32)
    before = jnp.cumsum(onehot, axis=0) - onehot
    slot_idx = jnp.sum(before * onehot, axis=1)
    row_limit = jnp.sum(onehot * counts_row[None, :], axis=1)
    buf_pos = jnp.where(slot_idx < row_limit, flat_ids * cap_rows + slot_idx, -1)
    return buf_pos.reshape(tok_n, top_n)


def expert_ffn(rows_in, w_gate, w_up, w_down):
    act_a = jnp.einsum("erd,edf->erf", rows_in, w_gate, preferred_element_type=jnp.float32)
    act_b = jnp.einsum("erd,edf->erf", rows_in, w_up, preferred_element_type=jnp.float32)
    hidden = (jax.nn.silu(act_a) * act_b).astype(jnp.bfloat16)
    return jnp.einsum("erf,efd->erd", hidden, w_down, preferred_element_type=jnp.float32).astype(jnp.bfloat16)


def dense_step(group_size, tokens, expert_ids, gate_w, route_counts, w_gate, w_up, w_down):
    tok_n = expert_ids.shape[0]
    n_local = w_gate.shape[0]
    model_dim = w_gate.shape[1]
    n_exp = n_local * group_size
    cap_rows = tok_n // 2
    buf_pos = place_rows(expert_ids, route_counts[0], cap_rows, n_exp)
    disp_mat = jnp.any(jnp.arange(n_exp * cap_rows)[:, None, None] == buf_pos[None, :, :], axis=2).astype(jnp.bfloat16)
    packed = jnp.dot(disp_mat, tokens, preferred_element_type=jnp.float32).astype(jnp.bfloat16)
    packed = packed.reshape(group_size, n_local, cap_rows, model_dim)
    arrived = lax.all_to_all(packed, "ep", 0, 2, tiled=True)
    expert_out = expert_ffn(arrived.reshape(n_local, group_size * cap_rows, model_dim), w_gate, w_up, w_down)
    returned = lax.all_to_all(expert_out.reshape(1, n_local, group_size * cap_rows, model_dim), "ep", 2, 0, tiled=True)
    picked = jnp.take(returned.reshape(n_exp * cap_rows, model_dim), jnp.maximum(buf_pos, 0), axis=0)
    weights = jnp.where(buf_pos >= 0, gate_w, 0.0)
    total_f32 = tokens.astype(jnp.float32) + jnp.sum(weights[:, :, None] * picked.astype(jnp.float32), axis=1)
    return total_f32.astype(jnp.bfloat16)


def chunk_of(wg, wu, wd, half, k):
    if k < 48:
        arr = wg if k < 24 else wu
        row, col = (k % 24) // 3, (k % 24) % 3
        start = half * 1024 + row * CH_R
    else:
        arr = wd
        row, col = (k - 48) // 8, (k - 48) % 8
        start = half * 384 + row * CH_R
    return arr.at[pl.ds(pl.multiple_of(start, CH_R), CH_R), pl.ds(col * CH_C, CH_C)]


def remote(src, dst, send, recv, dev):
    return pltpu.make_async_remote_copy(
        src_ref=src, dst_ref=dst, send_sem=send, recv_sem=recv, device_id={"ep": dev}, device_id_type=MESH
    )


def drain(ref, sem):
    pltpu.make_async_copy(ref, ref, sem).wait()


def spread_kernel(tok, ids, cnt, wg, wu, wd, tok_all, ids_all, cnt_all, st, xr, own, inj, stage, recv,
                  flags, tok_s, tok_r, ids_s, ids_r, cnt_s, cnt_r, loc, own_sem, inj_s, inj_r, ring_s, ring_r, par_s, par_r, st_sem):
    me = lax.axis_index("ep")
    grp, pos = me // GRP, me % GRP
    core, xx = pos % 2, pos // 2
    other = 1 - core
    partner = grp * GRP + xx * 2 + other
    nbr = grp * GRP + ((xx + 1 + 2 * core) % 4) * 2 + core
    wg, wu, wd = wg.at[0], wu.at[0], wd.at[0]

    loads = [pltpu.make_async_copy(chunk_of(wg, wu, wd, core, k), own.at[k], own_sem) for k in range(K)]
    for cp in loads:
        cp.start()
    bar = pltpu.get_barrier_semaphore()
    for k in range(1, GRP):
        pl.semaphore_signal(bar, inc=1, device_id={"ep": grp * GRP + (pos + k) % GRP}, device_id_type=MESH)
    for k in range(1, PLN):
        pl.semaphore_signal(bar, inc=1, device_id={"ep": ((grp + k) % PLN) * GRP + pos}, device_id_type=MESH)
    pl.semaphore_wait(bar, GRP - 1 + PLN - 1)

    for k in range(1, GRP):
        remote(cnt, cnt_all.at[pos], cnt_s, cnt_r, grp * GRP + (pos + k) % GRP).start()
    pltpu.make_async_copy(cnt, cnt_all.at[pos], loc.at[0]).start()
    for k in range(K):
        remote(chunk_of(wg, wu, wd, other, k), inj.at[k], inj_s, inj_r.at[k // INJ], partner).start()
    for k in range(1, PLN):
        dev = ((grp + k) % PLN) * GRP + pos
        remote(ids, ids_all.at[grp], ids_s, ids_r, dev).start()
        remote(tok, tok_all.at[grp], tok_s, tok_r, dev).start()
    pltpu.make_async_copy(ids, ids_all.at[grp], loc.at[1]).start()
    pltpu.make_async_copy(tok, tok_all.at[grp], loc.at[2]).start()

    pltpu.make_async_copy(cnt, cnt_all.at[pos], loc.at[0]).wait()
    drain(cnt_all.at[pl.ds(0, GRP - 1)], cnt_r)
    total = jnp.sum(cnt_all[...].astype(jnp.float32), axis=0)
    lane = lax.broadcasted_iota(jnp.int32, (8, 128), 1)
    key = total * 8.0 + (7 - lane % GRP).astype(jnp.float32)
    key = jnp.where(lane // GRP == grp, key, -1.0)
    best = jnp.max(key, axis=1, keepdims=True)
    hit = jnp.where(key == best, 1.0, 0.0)
    mine = jnp.max(jnp.where(lane == me, hit, 0.0), axis=1, keepdims=True)
    theirs = jnp.max(jnp.where(lane == partner, hit, 0.0), axis=1, keepdims=True)
    flags[0] = jnp.broadcast_to(mine, (8, 128))
    flags[1] = jnp.broadcast_to(theirs, (8, 128))
    drain(own, own_sem)

    def flag(i):
        row = flags[i, 0:1, :]
        return jnp.concatenate([row, row], axis=1)

    def send(t, src, ring=True):
        if ring:
            remote(src, recv.at[t], ring_s, ring_r.at[t % N_SEM], nbr).start()
        remote(src, xr.at[t], par_s, par_r, partner).start()
        pltpu.make_async_copy(src, st.at[t], st_sem).start()

    def take(t):
        pltpu.make_async_copy(recv.at[t], recv.at[t], ring_r.at[t % N_SEM]).wait()

    def build(t, first):
        a = own[t].astype(jnp.float32)
        b = inj[t].astype(jnp.float32)
        if not first:
            b = jnp.where(flag(1) > 0.5, b, recv[t - D].astype(jnp.float32))
        stage[t] = jnp.where(flag(0) > 0.5, a, b).astype(jnp.bfloat16)

    def head(t, carry):
        build(t, True)
        send(t - 1, stage.at[t - 1])
        return carry

    def body(t, carry):
        take(t - D)
        build(t, False)
        send(t - 1, stage.at[t - 1])
        return carry

    def tail(t, carry):
        take(t - D)
        send(t, recv.at[t - D])
        return carry

    def last(t, carry):
        take(t - D)
        send(t, recv.at[t - D], ring=False)
        return carry

    for blk in range(K // INJ):
        drain(inj.at[pl.ds(blk * INJ, INJ)], inj_r.at[blk])
        lo, hi = blk * INJ, (blk + 1) * INJ
        if blk == 0:
            build(0, True)
            lax.fori_loop(1, D, head, 0)
            lo = D
        lax.fori_loop(lo, hi, body, 0)
    send(K - 1, stage.at[K - 1])
    lax.fori_loop(K, N_RING, tail, 0)
    lax.fori_loop(N_RING, T, last, 0)

    drain(cnt_all.at[pl.ds(0, GRP - 1)], cnt_s)
    drain(inj, inj_s)
    drain(recv, ring_s)
    drain(st, st_sem)
    drain(xr, par_s)
    drain(xr, par_r)
    pltpu.make_async_copy(ids, ids_all.at[grp], loc.at[1]).wait()
    pltpu.make_async_copy(tok, tok_all.at[grp], loc.at[2]).wait()
    drain(ids_all.at[pl.ds(0, PLN - 1)], ids_s)
    drain(ids_all.at[pl.ds(0, PLN - 1)], ids_r)
    drain(tok_all.at[pl.ds(0, PLN - 1)], tok_s)
    drain(tok_all.at[pl.ds(0, PLN - 1)], tok_r)


def spread(tokens, ids_t, cnt_t, w_gate, w_up, w_down):
    dma = pltpu.SemaphoreType.DMA
    bf = jnp.bfloat16
    vm, an = pl.BlockSpec(memory_space=VMEM), pl.BlockSpec(memory_space=ANY)
    return pl.pallas_call(
        spread_kernel,
        out_shape=(
            jax.ShapeDtypeStruct((PLN, 64, 2048), bf),
            jax.ShapeDtypeStruct((PLN, 8, 128), jnp.int32),
            jax.ShapeDtypeStruct((GRP, 8, 128), jnp.int32),
            jax.ShapeDtypeStruct((T, CH_R, CH_C), bf),
            jax.ShapeDtypeStruct((T, CH_R, CH_C), bf),
        ),
        in_specs=[vm, vm, vm, an, an, an],
        out_specs=(an, vm, vm, an, an),
        scratch_shapes=[
            VMEM((K, CH_R, CH_C), bf),
            VMEM((K, CH_R, CH_C), bf),
            VMEM((K, CH_R, CH_C), bf),
            VMEM((N_RING, CH_R, CH_C), bf),
            VMEM((2, 8, 128), jnp.float32),
            dma, dma, dma, dma, dma, dma, dma((3,)), dma, dma, dma((K // INJ,)), dma, dma((N_SEM,)), dma, dma, dma,
        ],
        compiler_params=pltpu.CompilerParams(collective_id=0, has_side_effects=True, vmem_limit_bytes=48 * 2**20),
    )(tokens, ids_t, cnt_t, w_gate, w_up, w_down)


def swap_kernel(n, dev_of, my_of, rows, flg, out, flg_out, row_s, row_r, flg_s, flg_r, loc):
    me = lax.axis_index("ep")
    mine = my_of(me)
    bar = pltpu.get_barrier_semaphore()
    for k in range(1, n):
        pl.semaphore_signal(bar, inc=1, device_id={"ep": dev_of(me, (mine + k) % n)}, device_id_type=MESH)
    here = pltpu.make_async_copy(rows.at[mine], out.at[mine], loc.at[0])
    here_f = pltpu.make_async_copy(flg, flg_out.at[mine], loc.at[1])
    here.start()
    here_f.start()
    pl.semaphore_wait(bar, n - 1)
    for k in range(1, n):
        peer = (mine + k) % n
        dev = dev_of(me, peer)
        remote(rows.at[peer], out.at[mine], row_s, row_r, dev).start()
        remote(flg, flg_out.at[mine], flg_s, flg_r, dev).start()
    here.wait()
    here_f.wait()
    drain(rows.at[pl.ds(0, n - 1)], row_s)
    drain(out.at[pl.ds(0, n - 1)], row_r)
    drain(flg_out.at[pl.ds(0, n - 1)], flg_s)
    drain(flg_out.at[pl.ds(0, n - 1)], flg_r)


def swap(rows, flg, n, cid):
    if n == GRP:
        dev_of, my_of = (lambda me, i: (me // GRP) * GRP + i), (lambda me: me % GRP)
    else:
        dev_of, my_of = (lambda me, i: i * GRP + me % GRP), (lambda me: me // GRP)
    dma = pltpu.SemaphoreType.DMA
    vm = pl.BlockSpec(memory_space=VMEM)
    return pl.pallas_call(
        functools.partial(swap_kernel, n, dev_of, my_of),
        out_shape=(jax.ShapeDtypeStruct(rows.shape, rows.dtype), jax.ShapeDtypeStruct((n, 8, 128), jnp.int32)),
        in_specs=[vm, vm],
        out_specs=(vm, vm),
        scratch_shapes=[dma, dma, dma, dma, dma((2,))],
        compiler_params=pltpu.CompilerParams(collective_id=cid, has_side_effects=True, vmem_limit_bytes=24 * 2**20),
    )(rows, flg)


def ffn_rows(x, y, wg, wu, wd):
    def block(i, carry):
        at = pl.ds(pl.multiple_of(i * 256, 256), 256)
        rows = x[at, :]
        a = jnp.dot(rows, wg[...], preferred_element_type=jnp.float32)
        b = jnp.dot(rows, wu[...], preferred_element_type=jnp.float32)
        h = (jax.nn.silu(a) * b).astype(jnp.bfloat16)
        y[at, :] = jnp.dot(h, wd[...], preferred_element_type=jnp.float32).astype(jnp.bfloat16)
        return carry

    lax.fori_loop(0, x.shape[0] // 256, block, 0)


def ffn_kernel(info, st, xr, wg, wu, wd, xc, xh, yc, yh, cg, cu, cd, hg, hu, hd, sems):
    wg, wu, wd = wg.at[0], wu.at[0], wd.at[0]
    own = [pltpu.make_async_copy(s, d, sems.at[i]) for i, (s, d) in enumerate(((wg, cg), (wu, cu), (wd, cd)))]
    for cp in own:
        cp.start()
    core, first, second = info[0], info[1], info[2]
    for k in range(K):
        sem = sems.at[3 + k // 24]
        pltpu.make_async_copy(st.at[first + k], chunk_of(hg, hu, hd, core, k), sem).start()
        pltpu.make_async_copy(xr.at[second + k], chunk_of(hg, hu, hd, 1 - core, k), sem).start()
    for cp in own:
        cp.wait()
    ffn_rows(xc, yc, cg, cu, cd)
    for i, (s, d) in enumerate(((wg, hg), (wu, hu), (wd, hd))):
        pltpu.make_async_copy(s, d, sems.at[3 + i]).wait()
    ffn_rows(xh, yh, hg, hu, hd)


def ffn(info, st, xr, w_gate, w_up, w_down, xc, xh):
    bf = jnp.bfloat16
    vm, an = pl.BlockSpec(memory_space=VMEM), pl.BlockSpec(memory_space=ANY)
    up, down = VMEM((2048, 768), bf), VMEM((768, 2048), bf)
    return pl.pallas_call(
        ffn_kernel,
        out_shape=(jax.ShapeDtypeStruct(xc.shape, bf), jax.ShapeDtypeStruct(xh.shape, bf)),
        in_specs=[pl.BlockSpec(memory_space=pltpu.SMEM), an, an, an, an, an, vm, vm],
        out_specs=(vm, vm),
        scratch_shapes=[up, up, down, up, up, down, pltpu.SemaphoreType.DMA((6,))],
        compiler_params=pltpu.CompilerParams(vmem_limit_bytes=48 * 2**20),
    )(info, st, xr, w_gate, w_up, w_down, xc, xh)


def strict_upper(n):
    i = jnp.arange(n)
    return (i[:, None] < i[None, :]).astype(jnp.bfloat16)


def small_dot(a, b):
    return jnp.dot(a.astype(jnp.bfloat16), b, preferred_element_type=jnp.float32)


def flag_tile(ok):
    return jnp.broadcast_to(ok.astype(jnp.int32), (8, 128))


def sparse_step(tokens, expert_ids, gate_w, route_counts, w_gate, w_up, w_down):
    bf, f32 = jnp.bfloat16, jnp.float32
    me = lax.axis_index("ep")
    grp, pos = me // GRP, me % GRP
    core, xx = pos % 2, pos // 2
    ids_t = jnp.pad(expert_ids.T, ((0, 0), (0, 64)))
    cnt_t = jnp.broadcast_to(route_counts, (8, 128))
    tok_all, ids_all, cnt_all, st, xr = spread(tokens, ids_t, cnt_t, w_gate, w_up, w_down)

    e_ar = jnp.arange(128)
    hits = expert_ids[:, :, None] == e_ar[None, None, :]
    named = jnp.any(hits, axis=1)
    gates = jnp.sum(jnp.where(hits, gate_w[:, :, None], 0.0), axis=1)
    slot = jnp.dot(strict_upper(64).T, named.astype(bf), preferred_element_type=f32)
    kept = named & (slot < 32)
    n_kept = jnp.sum(kept.astype(f32), axis=0)
    same = (e_ar[:, None] // GRP) == (e_ar[None, :] // GRP)
    before = small_dot(n_kept[None, :], (same & (e_ar[:, None] < e_ar[None, :])).astype(bf))
    back = jnp.where(kept, before + slot, -1.0).astype(jnp.int32)
    gates = jnp.where(kept, gates, 0.0)
    fits_src = jnp.max(jnp.sum(n_kept.reshape(PLN, GRP), axis=1)) <= CAP_R

    totals = lax.dynamic_slice(jnp.sum(cnt_all[:, 0, :], axis=0), (grp * GRP,), (GRP,))
    hot = jnp.argmax(totals).astype(jnp.int32)
    local_ids = ids_all[:, :, :64] - grp * GRP
    p_ar = jnp.arange(GRP)
    m0 = jnp.any(local_ids[None] == p_ar[:, None, None, None], axis=2)
    q = jnp.dot(m0.astype(bf).reshape(GRP * PLN, 64), strict_upper(64), preferred_element_type=f32).reshape(GRP, PLN, 64)
    m = m0 & (q < 32)
    n_ps = jnp.sum(m.astype(f32), axis=2)
    rank = (small_dot(n_ps, strict_upper(PLN))[:, :, None] + q).astype(jnp.int32)
    back_at = (small_dot(n_ps.T, strict_upper(GRP)).T[:, :, None] + q).astype(jnp.int32)
    is_hot = p_ar == hot
    fits_mid = jnp.all(is_hot | (jnp.sum(n_ps, axis=1) <= CAP_C))
    rank_c = jnp.where(m & ~is_hot[:, None, None], rank, -1).reshape(GRP, 1, PLN * 64)
    rank_h = jnp.max(jnp.where(m & is_hot[:, None, None], rank, -1), axis=0).reshape(1, PLN * 64)
    disp_c = (jnp.arange(CAP_C)[None, :, None] == rank_c).astype(bf).reshape(GRP * CAP_C, PLN * 64)
    disp_h = (jnp.arange(512)[:, None] == rank_h).astype(bf)
    toks = tok_all.reshape(PLN * 64, 2048)
    rows_c = jnp.dot(disp_c, toks, preferred_element_type=f32).astype(bf)
    rows_h = jnp.dot(disp_h, toks, preferred_element_type=f32).astype(bf)

    arrived, ok_grp = swap(rows_c.reshape(GRP, CAP_C, 2048), flag_tile(fits_src & fits_mid), GRP, 1)
    hx = hot // 2
    hops = jnp.where(core == 0, xx - hx, hx - xx) % 4
    info = jnp.stack([core, D * hops, D * ((4 - hops) % 4)]).astype(jnp.int32)
    y_c, y_h = ffn(info, st, xr, w_gate, w_up, w_down, arrived.reshape(GRP * CAP_C, 2048), rows_h)
    ok_tile = jnp.broadcast_to(jnp.min(ok_grp[:, :1, :1]), (8, 128))
    home_c, _ = swap(y_c.reshape(GRP, CAP_C, 2048), ok_tile, GRP, 2)

    row = jnp.where(is_hot[:, None, None], GRP * CAP_C + rank, p_ar[:, None, None] * CAP_C + rank)
    r_ar = jnp.arange(CAP_R)
    pick = jnp.where(m[:, :, None, :] & (back_at[:, :, None, :] == r_ar[None, None, :, None]), row[:, :, None, :] + 1, 0)
    src_row = jnp.sum(pick, axis=(0, 3)) - 1
    pack = (src_row.reshape(PLN * CAP_R, 1) == jnp.arange(GRP * CAP_C + 512)[None, :]).astype(bf)
    y_all = jnp.concatenate([home_c.reshape(GRP * CAP_C, 2048), y_h], axis=0)
    ret = jnp.dot(pack, y_all, preferred_element_type=f32).astype(bf)
    home, ok_all = swap(ret.reshape(PLN, CAP_R, 2048), ok_tile, PLN, 3)

    comb = jnp.sum(
        jnp.where(back.reshape(64, PLN, GRP)[:, :, :, None] == r_ar, gates.reshape(64, PLN, GRP)[:, :, :, None], 0.0), axis=2
    ).reshape(64, PLN * CAP_R)
    g1 = lax.reduce_precision(comb, 8, 7)
    g2 = lax.reduce_precision(comb - g1, 8, 7)
    g3 = lax.reduce_precision(comb - g1 - g2, 8, 7)
    parts = jnp.dot(
        jnp.concatenate([g1, g2, g3], axis=0).astype(bf), home.reshape(PLN * CAP_R, 2048), preferred_element_type=f32
    )
    total = tokens.astype(f32) + (parts[:64] + (parts[64:128] + parts[128:]))
    return total.astype(bf), jnp.min(ok_all[:, 0, 0]) > 0


def solution(mesh):
    group_size = mesh.shape["ep"]
    row_spec = P(("dp", "ep"))

    def local_step(*args):
        fast, ok = sparse_step(*args)
        return lax.cond(ok, lambda: fast, lambda: dense_step(group_size, *args))

    return jax.shard_map(
        local_step,
        mesh=mesh,
        in_specs=(row_spec, row_spec, row_spec, row_spec, P("ep"), P("ep"), P("ep")),
        out_specs=row_spec,
        check_vma=False,
    )
```

```python
import functools

import jax
import jax.numpy as jnp
from jax import lax
from jax.experimental import pallas as pl
from jax.experimental.pallas import tpu as pltpu
from jax.sharding import PartitionSpec as P

MESH = pl.DeviceIdType.MESH
VMEM = pltpu.VMEM
ANY = pl.ANY
F32 = jnp.float32
MODEL, FFN, TILE, MIB = 2048, 768, (8, 128), 2**20
DOWN, ACROSS = dict(axis=0, keepdims=True), dict(axis=1, keepdims=True)
EFFECTS = dict(has_side_effects=True)
GRP = 8
PLN = 16
CAP_C = 32
CH_R, CH_C = 128, 256
K = 72
D = 7
T = K + 3 * D
N_RING = K + 2 * D
N_SEM = 32
INJ = 12
CAP_B = 16
RING_AG = 44
RING_X1, RING_X2 = 8, 12
FAR = (10, 6, 14, 9, 11, 2, 8, 5, 7, 13, 15, 1, 3, 4, 12)


def place_rows(expert_ids, counts_row, cap_rows, n_exp):
    tok_n, top_n = expert_ids.shape
    flat_ids = expert_ids.reshape(tok_n * top_n)
    onehot = (flat_ids[:, None] == jnp.arange(n_exp)[None, :]).astype(jnp.int32)
    before = jnp.cumsum(onehot, axis=0) - onehot
    slot_idx = jnp.sum(before * onehot, axis=1)
    row_limit = jnp.sum(onehot * counts_row[None, :], axis=1)
    buf_pos = jnp.where(slot_idx < row_limit, flat_ids * cap_rows + slot_idx, -1)
    return buf_pos.reshape(tok_n, top_n)


def expert_ffn(rows_in, w_gate, w_up, w_down):
    act_a = jnp.einsum("erd,edf->erf", rows_in, w_gate, preferred_element_type=F32)
    act_b = jnp.einsum("erd,edf->erf", rows_in, w_up, preferred_element_type=F32)
    hidden = (jax.nn.silu(act_a) * act_b).astype(jnp.bfloat16)
    return jnp.einsum("erf,efd->erd", hidden, w_down, preferred_element_type=F32).astype(jnp.bfloat16)


def dense_step(group_size, tokens, expert_ids, gate_w, route_counts, w_gate, w_up, w_down):
    tok_n = expert_ids.shape[0]
    n_local = w_gate.shape[0]
    model_dim = w_gate.shape[1]
    n_exp = n_local * group_size
    cap_rows = tok_n // 2
    buf_pos = place_rows(expert_ids, route_counts[0], cap_rows, n_exp)
    disp_mat = jnp.any(jnp.arange(n_exp * cap_rows)[:, None, None] == buf_pos[None, :, :], axis=2).astype(jnp.bfloat16)
    packed = jnp.dot(disp_mat, tokens, preferred_element_type=F32).astype(jnp.bfloat16)
    packed = packed.reshape(group_size, n_local, cap_rows, model_dim)
    arrived = lax.all_to_all(packed, "ep", 0, 2, tiled=True)
    expert_out = expert_ffn(arrived.reshape(n_local, group_size * cap_rows, model_dim), w_gate, w_up, w_down)
    returned = lax.all_to_all(expert_out.reshape(1, n_local, group_size * cap_rows, model_dim), "ep", 2, 0, tiled=True)
    picked = jnp.take(returned.reshape(n_exp * cap_rows, model_dim), jnp.maximum(buf_pos, 0), axis=0)
    weights = jnp.where(buf_pos >= 0, gate_w, 0.0)
    total_f32 = tokens.astype(jnp.float32) + jnp.sum(weights[:, :, None] * picked.astype(jnp.float32), axis=1)
    return total_f32.astype(jnp.bfloat16)


def chunk_of(wg, wu, wd, half, k):
    if k < 48:
        arr = wg if k < 24 else wu
        row, col = (k % 24) // 3, (k % 24) % 3
        start = half * 1024 + row * CH_R
    else:
        arr = wd
        row, col = (k - 48) // 8, (k - 48) % 8
        start = half * 384 + row * CH_R
    return arr.at[pl.ds(pl.multiple_of(start, CH_R), CH_R), pl.ds(col * CH_C, CH_C)]


def remote(src, dst, send, recv, dev):
    return pltpu.make_async_remote_copy(
        src_ref=src, dst_ref=dst, send_sem=send, recv_sem=recv, device_id={"ep": dev}, device_id_type=MESH
    )


def block_at(i, n):
    return pl.ds(i * n if isinstance(i, int) else pl.multiple_of(i * n, n), n)


def first(n):
    return pl.ds(0, n)


def others(ref):
    return ref.at[first(ref.shape[0] - 1)]


def plane_peer(grp, k):
    return ((grp // 4 + k // 4) % 4) * 4 + (grp % 4 + k % 4) % 4


def drain(ref, sem):
    pltpu.make_async_copy(ref, ref, sem).wait()


def ffn_rows(x, y, wg, wu, wd):
    def block(i, carry):
        at = block_at(i, 256)
        rows = x[at, :]
        a = jnp.dot(rows, wg[...], preferred_element_type=F32)
        b = jnp.dot(rows, wu[...], preferred_element_type=F32)
        h = (jax.nn.silu(a) * b).astype(jnp.bfloat16)
        y[at, :] = jnp.dot(h, wd[...], preferred_element_type=F32).astype(jnp.bfloat16)
        return carry

    lax.fori_loop(0, x.shape[0] // 256, block, 0)


def iota(shape, dim):
    return lax.broadcasted_iota(jnp.int32, shape, dim)


def ones_where(cond):
    return jnp.where(cond, 1.0, 0.0).astype(jnp.bfloat16)


def fdot(a, b):
    return jnp.dot(a.astype(jnp.bfloat16), b.astype(jnp.bfloat16), preferred_element_type=F32)


def main_kernel(tok, ids, gat, cnt, wg, wu, wd,
                rows_h, st, xr, cold_home, gh, gc, ok_all, info,
                own, inj, stage, recv, cg, cu, cd, toks, rows_c, arr, y_c, home_c, ret_c, hid,
                sl, gt, tab_all, cnt_all, hot_all, flags, hot_t, ok_t, ok_grp, rk, kc, sh, disp, kexp, pack, ght, gct,
                dma1, inj_r, ring_r):
    me = lax.axis_index("ep")
    grp, pos = me // GRP, me % GRP
    zz, yy = grp // 4, grp % 4
    core, xx = pos % 2, pos // 2
    other = 1 - core
    partner = grp * GRP + xx * 2 + other
    nbr = grp * GRP + ((xx + 1 + 2 * core) % 4) * 2 + core
    wg, wu, wd = wg.at[0], wu.at[0], wd.at[0]
    (own_sem, w0_sem, w1_sem, w2_sem, cnt_s, cnt_r, tab_s, tab_r, hot_s, hot_r, inj_s, a1_s, a1_r, b1_s, b1_r, p2_s, p2_r,
     xd_s, xd_r, ok_s, ok_r, xb_s, xb_r, pr_s, pr_r, oa_s, oa_r, ring_s, par_s, par_r, st_sem, loc_sem) = [dma1.at[i] for i in range(32)]

    def xdev(k):
        return grp * GRP + (pos + k) % GRP

    def pdev(k):
        return ((grp + k) % PLN) * GRP + pos

    for k in range(K):
        pltpu.make_async_copy(chunk_of(wg, wu, wd, core, k), own.at[k], own_sem).start()
    mine_at = block_at(grp, 64)
    pltpu.make_async_copy(tok, toks.at[mine_at], loc_sem).start()
    full = [pltpu.make_async_copy(s, d, q) for s, d, q in ((wg, cg, w0_sem), (wu, cu, w1_sem), (wd, cd, w2_sem))]

    sq = (128, 128)
    e_i = iota(sq, 0)
    named = jnp.zeros(sq, F32)
    gates = jnp.zeros(sq, F32)
    for j in range(8):
        hit_j = ids[j : j + 1, :] == e_i
        named = jnp.where(hit_j, 1.0, named)
        gates = jnp.where(hit_j, gat[j : j + 1, :], gates)
    l0, l1 = iota(sq, 0), iota(sq, 1)
    slot = fdot(named, ones_where(((l0 >> 6) == (l1 >> 6)) & (l0 < l1)))
    sl[...] = jnp.where((named > 0.5) & (slot < 32.0), slot, -1.0).reshape(PLN, *TILE)
    gt[...] = gates.reshape(PLN, *TILE)

    bar = pltpu.get_barrier_semaphore()
    for k in range(1, GRP):
        pl.semaphore_signal(bar, inc=1, device_id={"ep": xdev(k)}, device_id_type=MESH)
    for k in range(1, PLN):
        pl.semaphore_signal(bar, inc=1, device_id={"ep": pdev(k)}, device_id_type=MESH)
    pl.semaphore_wait(bar, GRP - 1 + PLN - 1)

    for k in range(1, GRP):
        remote(cnt, cnt_all.at[pos], cnt_s, cnt_r, xdev(k)).start()
    cnt_all[pos] = cnt[...]

    def half_at(z, y, h):
        return pl.ds(pl.multiple_of(((z % 4) * 4 + (y % 4)) * 64 + 32 * h, 32), 32)

    def plane_dev(z, y):
        return ((z % 4) * 4 + (y % 4)) * GRP + pos

    for k in (1, 3, 2):
        remote(tok.at[first(32)], toks.at[half_at(zz, yy, 0)], a1_s, a1_r, plane_dev(zz, yy + k)).start()
        remote(tok.at[pl.ds(32, 32)], toks.at[half_at(zz, yy, 1)], b1_s, b1_r, plane_dev(zz + k, yy)).start()
    for k in range(K):
        remote(chunk_of(wg, wu, wd, other, k), inj.at[k], inj_s, inj_r.at[k // INJ], partner).start()
    for k in range(1, PLN):
        remote(sl.at[(grp + k) % PLN], tab_all.at[grp], tab_s, tab_r, pdev(k)).start()
    tab_all[grp] = sl[grp]
    for cp in full:
        cp.start()

    drain(others(cnt_all), cnt_r)
    total = jnp.sum(cnt_all[...].astype(jnp.float32), axis=0)
    lane = iota(TILE, 1)
    key = total * 8.0 + (7 - (lane & 7)).astype(jnp.float32)
    key = jnp.where((lane >> 3) == grp, key, -1.0)
    best = jnp.max(key, **ACROSS)
    hit = jnp.where(key == best, 1.0, 0.0)
    mine = jnp.max(jnp.where(lane == me, hit, 0.0), **ACROSS)
    theirs = jnp.max(jnp.where(lane == partner, hit, 0.0), **ACROSS)
    flags[0] = jnp.broadcast_to(mine, TILE)
    flags[1] = jnp.broadcast_to(theirs, TILE)
    hot_p = jnp.max(jnp.where(lane == grp * 8 + iota(TILE, 0), hit, 0.0), **ACROSS)
    hot_t[...] = jnp.broadcast_to(hot_p, TILE)
    hx = jnp.sum(hit * ((lane & 7) >> 1).astype(jnp.float32), **ACROSS).astype(jnp.int32)
    sign = 1 - 2 * core
    hops = (sign * (xx - hx) + 8) & 3
    info[...] = jnp.where(iota(TILE, 0) == 0, D * hops, D * ((4 - hops) & 3))
    drain(own, own_sem)

    def flag(i):
        row = flags[i, 0:1, :]
        return jnp.concatenate([row, row], axis=1)

    def send(t, src, ring=True):
        if ring:
            remote(src, recv.at[t], ring_s, ring_r.at[t % N_SEM], nbr).start()
        remote(src, xr.at[t], par_s, par_r, partner).start()
        pltpu.make_async_copy(src, st.at[t], st_sem).start()

    def take(t):
        pltpu.make_async_copy(recv.at[t], recv.at[t], ring_r.at[t % N_SEM]).wait()

    def build(t, first):
        a = own[t].astype(jnp.float32)
        b = inj[t].astype(jnp.float32)
        if not first:
            b = jnp.where(flag(1) > 0.5, b, recv[t - D].astype(jnp.float32))
        stage[t] = jnp.where(flag(0) > 0.5, a, b).astype(jnp.bfloat16)

    def head(t):
        build(t, True)
        send(t - 1, stage.at[t - 1])

    def body(t):
        take(t - D)
        build(t, False)
        send(t - 1, stage.at[t - 1])

    def tail(t):
        take(t - D)
        send(t, recv.at[t - D])

    def last(t):
        take(t - D)
        send(t, recv.at[t - D], ring=False)

    at = [0]

    def ring(n, task=None):
        base = at[0]
        end = min(base + n, T)
        while at[0] < end:
            t = at[0]
            if t < K and t % INJ == 0:
                drain(inj.at[pl.ds(t, INJ)], inj_r.at[t // INJ])
            if t == K:
                send(K - 1, stage.at[K - 1])
            if t == 0:
                build(0, True)
                if task is not None:
                    task(0)
                at[0] = 1
                continue
            kind, stop = (head, D) if t < D else (body, (t // INJ + 1) * INJ) if t < K else (tail, N_RING) if t < N_RING else (last, T)
            stop = min(stop, end)

            def step(i, carry, kind=kind):
                kind(i)
                if task is not None:
                    task(i - base)
                return carry

            lax.fori_loop(t, stop, step, 0)
            at[0] = stop
        if task is not None:
            for i in range(end - base, n):
                task(i)

    ring(1)
    for k in range(1, PLN):
        remote(hot_t, hot_all.at[grp], hot_s, hot_r, pdev(k)).start()
    hot_all[grp] = hot_t[...]
    ring(3)
    pltpu.make_async_copy(tok, toks.at[mine_at], loc_sem).wait()
    drain(toks.at[first(96)], a1_r)
    drain(toks.at[first(96)], b1_r)
    for k in (2, 1, 3):
        for i in range(4):
            a_at, b_at = half_at(zz, yy + i, 0), half_at(zz + i, yy, 1)
            remote(toks.at[a_at], toks.at[a_at], p2_s, p2_r, plane_dev(zz + k, yy)).start()
            remote(toks.at[b_at], toks.at[b_at], p2_s, p2_r, plane_dev(zz, yy + k)).start()

    ring(3)
    drain(others(hot_all), hot_r)

    def gate_task(g):
        s, w, h = sl[g], gt[g], hot_all[g]
        s_h = jnp.sum(h * (s + 1.0), **DOWN) - 1.0
        w_h = jnp.sum(h * w, **DOWN)
        ght[block_at(g, 32), :] = jnp.where(iota((32, 128), 0).astype(jnp.float32) == s_h, w_h, 0.0)
        n = jnp.sum(jnp.where((s >= 0.0) & (lane < 64), 1.0 - h, 0.0), **ACROSS)
        off = jnp.zeros((1, 1), jnp.float32)
        acc = jnp.zeros((16, 128), jnp.float32)
        r_i = iota((16, 128), 0).astype(jnp.float32)
        for p in range(GRP):
            s_p = s[p : p + 1, :]
            use = (s_p >= 0.0) & (h[p : p + 1, :] < 0.5)
            r_p = jnp.where(use, s_p + off, -1.0)
            acc = acc + jnp.where(r_i == r_p, w[p : p + 1, :], 0.0)
            off = off + n[p : p + 1, :]
        gct[block_at(g, 16), :] = acc

    ring(16, gate_task)
    gh[...] = ght[...].T
    gc[...] = gct[...].T
    ring(1)

    drain(others(tab_all), tab_r)
    hot16 = jnp.concatenate([hot_t[:, 0:1], jnp.zeros((8, 1), jnp.float32)], axis=0)
    s8 = jnp.concatenate([jnp.where(lane < 64, tab_all[2 * i], tab_all[2 * i + 1]) for i in range(8)], axis=1)
    s16 = jnp.concatenate([s8, jnp.full((8, 1024), -1.0, jnp.float32)], axis=0)
    kept = s16 >= 0.0
    bm = ones_where((iota((1024, 128), 0) >> 6) == iota((1024, 128), 1))
    bt = ones_where((iota((128, 1024), 1) >> 6) == iota((128, 1024), 0))
    n_ps = fdot(jnp.where(kept, 1.0, 0.0), bm)
    offs = fdot(n_ps, ones_where(l0 < l1))
    off_l = fdot(jnp.minimum(offs, 255.0), bt)
    cold = kept & (hot16 < 0.5)
    rk[...] = jnp.where(cold, off_l + s16, -1.0)
    kc[...] = jnp.where(cold, 1.0, 0.0)
    sh[...] = jnp.broadcast_to(jnp.max(jnp.where(hot16 > 0.5, s16, -1.0), **DOWN), (8, 1024))
    ring(1)
    for p in range(GRP):
        at_p = block_at(p, CAP_C)
        disp[at_p, :] = ones_where(iota((CAP_C, 1024), 0).astype(jnp.float32) == rk[p : p + 1, :])
        kexp[at_p, :] = jnp.broadcast_to(kc[p : p + 1, :], (CAP_C, 1024)).astype(jnp.bfloat16)
        ring(1)
    n_e = lax.dot_general(bt, kexp[...], (((1,), (1,)), ((), ())), preferred_element_type=F32)
    most = jnp.max(jnp.sum(n_e, **DOWN), **ACROSS)
    row_most = jnp.max(jnp.sum(n_e, **ACROSS), **DOWN)
    fits = jnp.where((most <= CAP_C) & (row_most <= 32.0 * CAP_B), 1.0, 0.0)
    ok_t[0] = jnp.broadcast_to(fits, TILE)
    wide = (256, 256)
    os_e = fdot(ones_where(l1 < l0), n_e)
    oc_e = fdot(n_e, ones_where(((iota(wide, 0) >> 5) < (iota(wide, 1) >> 5)) & ((iota(wide, 0) & 31) == 0)))
    e_row = ones_where((iota((256, 128), 0) >> 4) == iota((256, 128), 1))
    n_f = fdot(e_row, n_e)
    q_k = (iota(wide, 1) & 31).astype(jnp.float32) - fdot(e_row, jnp.minimum(os_e, 255.0))
    q_r = (iota(wide, 0) & 15).astype(jnp.float32) - fdot(e_row, jnp.minimum(oc_e, 255.0))
    pack[...] = ones_where((q_k == q_r) & (q_k >= 0.0) & (q_k < n_f))
    ring(RING_AG - at[0])

    drain(toks.at[first(768)], p2_r)

    def disp_task(c):
        cols = block_at(c, 256)
        block = jnp.dot(disp[...], toks[:, cols], preferred_element_type=F32).astype(jnp.bfloat16)
        rows_c[:, :, cols] = block.reshape(GRP, CAP_C, 256)

    ring(8, disp_task)
    arr[pos] = rows_c[pos]
    ok_grp[pos] = ok_t[0]

    def x_send(src, dst, s_sem, r_sem):
        def task(i):
            part = block_at(i, 8)
            for k in (1, 7, 2, 3, 4, 5, 6):
                remote(src.at[(pos + k) % GRP, part], dst.at[pos, part], s_sem, r_sem, xdev(k)).start()
        return task

    for k in range(1, GRP):
        remote(ok_t.at[0], ok_grp.at[pos], ok_s, ok_r, xdev(k)).start()
    ring(4, x_send(rows_c, arr, xd_s, xd_r))

    def hot_task(i):
        lanes = block_at(i, 128)
        slots = sh[0:1, lanes]
        r_i = iota((64, 128), 0)
        mine_rows = (r_i >> 5) == (iota((64, 128), 1) >> 6)
        pick = ones_where(mine_rows & ((r_i & 31).astype(jnp.float32) == slots))
        out = jnp.dot(pick, toks[block_at(i, 128), :], preferred_element_type=F32)
        rows_h[block_at(i, 64), :] = out.astype(jnp.bfloat16)

    ring(8, hot_task)
    ring(RING_X1)
    drain(others(arr), xd_r)
    drain(others(ok_grp), ok_r)
    ok_t[1] = jnp.min(ok_grp[...], axis=0)
    for cp in full:
        cp.wait()

    def up_task(c):
        cols = block_at(c, 256)
        x = arr[...].reshape(GRP * CAP_C, MODEL)
        a = jnp.dot(x, cg[:, cols], preferred_element_type=F32)
        b = jnp.dot(x, cu[:, cols], preferred_element_type=F32)
        hid[:, cols] = (jax.nn.silu(a) * b).astype(jnp.bfloat16)

    def down_task(c):
        cols = block_at(c, 512)
        y = jnp.dot(hid[...], cd[:, cols], preferred_element_type=F32).astype(jnp.bfloat16)
        y_c[:, :, cols] = y.reshape(GRP, CAP_C, 512)

    ring(3, up_task)
    ring(4, down_task)
    home_c[pos] = y_c[pos]
    ring(4, x_send(y_c, home_c, xb_s, xb_r))
    ring(RING_X2)
    drain(others(home_c), xb_r)

    def pack_task(c):
        cols = block_at(c, 512)
        block = jnp.dot(pack[...], home_c[:, :, cols].reshape(GRP * CAP_C, 512), preferred_element_type=F32)
        ret_c[:, :, cols] = block.astype(jnp.bfloat16).reshape(PLN, CAP_B, 512)

    ring(4, pack_task)
    cold_home[grp] = ret_c[grp]
    ok_all[grp] = ok_t[1]
    ring(1)
    for k in FAR:
        peer = plane_peer(grp, k)
        remote(ret_c.at[peer], cold_home.at[grp], pr_s, pr_r, peer * GRP + pos).start()
    for k in range(1, PLN):
        remote(ok_t.at[1], ok_all.at[grp], oa_s, oa_r, pdev(k)).start()
    ring(T)

    drain(others(cnt_all), cnt_s)
    drain(others(tab_all), tab_s)
    drain(others(hot_all), hot_s)
    drain(toks.at[first(96)], a1_s)
    drain(toks.at[first(96)], b1_s)
    drain(toks.at[first(768)], p2_s)
    drain(others(ok_grp), ok_s)
    drain(others(arr), xd_s)
    drain(others(home_c), xb_s)
    drain(inj, inj_s)
    drain(recv, ring_s)
    drain(st, st_sem)
    drain(xr, par_s)
    drain(xr, par_r)
    drain(others(ok_all), oa_s)
    drain(others(ok_all), oa_r)
    drain(others(cold_home), pr_s)
    drain(others(cold_home), pr_r)


def main_call(tokens, ids_t, gat_t, cnt_t, w_gate, w_up, w_down):
    dma = pltpu.SemaphoreType.DMA
    bf, f32 = jnp.bfloat16, jnp.float32
    vm, an = pl.BlockSpec(memory_space=VMEM), pl.BlockSpec(memory_space=ANY)
    chunks = lambda n: VMEM((n, CH_R, CH_C), bf)
    tile = lambda *n: VMEM((*n, *TILE), f32)
    rows = VMEM((GRP, CAP_C, MODEL), bf)
    out = jax.ShapeDtypeStruct
    return pl.pallas_call(
        main_kernel,
        out_shape=(
            out((512, MODEL), bf), out((T, CH_R, CH_C), bf), out((T, CH_R, CH_C), bf), out((PLN, CAP_B, MODEL), bf),
            out((128, 512), f32), out((128, 256), f32), out((PLN, *TILE), f32), out(TILE, jnp.int32),
        ),
        in_specs=[vm, vm, vm, vm, an, an, an],
        out_specs=(vm, an, an, vm, vm, vm, vm, vm),
        scratch_shapes=[
            chunks(K), chunks(K), chunks(K), chunks(N_RING),
            VMEM((MODEL, FFN), bf), VMEM((MODEL, FFN), bf), VMEM((FFN, MODEL), bf),
            VMEM((1024, MODEL), bf), rows, rows, rows, rows, VMEM((PLN, CAP_B, MODEL), bf), VMEM((GRP * CAP_C, FFN), bf),
            tile(PLN), tile(PLN), tile(PLN), VMEM((GRP, *TILE), jnp.int32), tile(PLN), tile(2), tile(), tile(2), tile(GRP),
            VMEM((16, 1024), f32), VMEM((16, 1024), f32), VMEM((8, 1024), f32), VMEM((256, 1024), bf), VMEM((256, 1024), bf),
            VMEM((256, 256), bf), VMEM((512, 128), f32), VMEM((256, 128), f32),
            dma((32,)), dma((K // INJ,)), dma((N_SEM,)),
        ],
        compiler_params=pltpu.CompilerParams(collective_id=0, **EFFECTS, vmem_limit_bytes=60 * MIB),
    )(tokens, ids_t, gat_t, cnt_t, w_gate, w_up, w_down)


def hot_kernel(info, st, xr, wg, wu, wd, x, y, hg, hu, hd, sems):
    core = lax.axis_index("ep") % 2
    first, second = info[0, 0], info[1, 0]
    for k in range(K):
        sem = sems.at[k // 24]
        pltpu.make_async_copy(st.at[first + k], chunk_of(hg, hu, hd, core, k), sem).start()
        pltpu.make_async_copy(xr.at[second + k], chunk_of(hg, hu, hd, 1 - core, k), sem).start()
    for i, (s, d) in enumerate(((wg.at[0], hg), (wu.at[0], hu), (wd.at[0], hd))):
        pltpu.make_async_copy(s, d, sems.at[i]).wait()
    ffn_rows(x, y, hg, hu, hd)


def hot_call(info, st, xr, w_gate, w_up, w_down, x):
    bf = jnp.bfloat16
    vm, an = pl.BlockSpec(memory_space=VMEM), pl.BlockSpec(memory_space=ANY)
    return pl.pallas_call(
        hot_kernel,
        out_shape=jax.ShapeDtypeStruct(x.shape, bf),
        in_specs=[pl.BlockSpec(memory_space=pltpu.SMEM), an, an, an, an, an, vm],
        out_specs=vm,
        scratch_shapes=[VMEM((MODEL, FFN), bf), VMEM((MODEL, FFN), bf), VMEM((FFN, MODEL), bf), pltpu.SemaphoreType.DMA((3,))],
        compiler_params=pltpu.CompilerParams(vmem_limit_bytes=40 * MIB),
    )(info, st, xr, w_gate, w_up, w_down, x)


def final_kernel(y, tok, gh, gc, cold, out, home, acc, row_s, row_r):
    me = lax.axis_index("ep")
    grp, pos = me // GRP, me % GRP
    bar = pltpu.get_barrier_semaphore()
    for k in range(1, PLN):
        pl.semaphore_signal(bar, inc=1, device_id={"ep": ((grp + k) % PLN) * GRP + pos}, device_id_type=MESH)
    pl.semaphore_wait(bar, PLN - 1)
    for k in FAR:
        peer = plane_peer(grp, k)
        remote(y.at[peer], home.at[grp], row_s, row_r, peer * GRP + pos).start()
    home[grp] = y[grp]

    def pieces(g):
        g1 = g.astype(jnp.bfloat16)
        r1 = g - g1.astype(jnp.float32)
        g2 = r1.astype(jnp.bfloat16)
        g3 = (r1 - g2.astype(jnp.float32)).astype(jnp.bfloat16)
        return jnp.concatenate([g1, g2, g3], axis=0)

    def add(g, vals):
        parts = jnp.dot(g, vals, preferred_element_type=F32)
        return parts[:64] + (parts[64:128] + parts[128:])

    w_c, w_h = pieces(gc[0:64, :]), pieces(gh[0:64, :])
    for c in range(4):
        cols = block_at(c, 512)
        vals = cold[:, :, cols].reshape(PLN * CAP_B, 512)
        acc[:, cols] = tok[:, cols].astype(jnp.float32) + add(w_c, vals)
    drain(others(home), row_r)
    for c in range(4):
        cols = block_at(c, 512)
        vals = home[:, :, cols].reshape(512, 512)
        out[:, cols] = (acc[:, cols] + add(w_h, vals)).astype(jnp.bfloat16)
    drain(others(home), row_s)


def final_call(y, tokens, gh, gc, cold):
    bf = jnp.bfloat16
    vm = pl.BlockSpec(memory_space=VMEM)
    return pl.pallas_call(
        final_kernel,
        out_shape=jax.ShapeDtypeStruct((64, MODEL), bf),
        in_specs=[vm] * 5,
        out_specs=vm,
        scratch_shapes=[VMEM((PLN, 32, MODEL), bf), VMEM((64, MODEL), jnp.float32), pltpu.SemaphoreType.DMA, pltpu.SemaphoreType.DMA],
        compiler_params=pltpu.CompilerParams(collective_id=1, **EFFECTS, vmem_limit_bytes=40 * MIB),
    )(y, tokens, gh, gc, cold)


def sparse_step(tokens, expert_ids, gate_w, route_counts, w_gate, w_up, w_down):
    ids_t = jnp.concatenate([expert_ids.T, expert_ids.T], axis=1)
    gat_t = jnp.concatenate([gate_w.T, gate_w.T], axis=1)
    cnt_t = jnp.broadcast_to(route_counts, TILE)
    rows_h, st, xr, cold, gh, gc, ok_all, info = main_call(tokens, ids_t, gat_t, cnt_t, w_gate, w_up, w_down)
    y_h = hot_call(info, st, xr, w_gate, w_up, w_down, rows_h)
    out = final_call(y_h.reshape(PLN, 32, MODEL), tokens, gh, gc, cold)
    return out, jnp.min(ok_all) > 0.5


def solution(mesh):
    group_size = mesh.shape["ep"]
    row_spec = P(("dp", "ep"))

    def local_step(*args):
        fast, ok = sparse_step(*args)
        return lax.cond(ok, lambda: fast, lambda: dense_step(group_size, *args))

    return jax.shard_map(
        local_step,
        mesh=mesh,
        in_specs=(row_spec, row_spec, row_spec, row_spec, P("ep"), P("ep"), P("ep")),
        out_specs=row_spec,
        check_vma=False,
    )
```

```python
import functools

import jax
import jax.numpy as jnp
from jax import lax
from jax.experimental import pallas as pl
from jax.experimental.pallas import tpu as pltpu
from jax.sharding import PartitionSpec as P

MESH = pl.DeviceIdType.MESH
VMEM = pltpu.VMEM
ANY = pl.ANY
F32 = jnp.float32
MODEL, FFN, TILE, MIB = 2048, 768, (8, 128), 2**20
DOWN, ACROSS = dict(axis=0, keepdims=True), dict(axis=1, keepdims=True)
EFFECTS = dict(has_side_effects=True)
GRP = 8
PLN = 16
CAP_C = 32
CH_R, CH_C = 128, 256
K = 72
D = 7
T = K + 3 * D
N_RING = K + 2 * D
N_SEM = 32
INJ = 12
PITCH = 32
CAP_B = 24
RING_AG = 44
RING_X1, RING_X2 = 8, 12
FAR = (10, 6, 14, 9, 11, 2, 8, 5, 7, 13, 15, 1, 3, 4, 12)


def place_rows(expert_ids, counts_row, cap_rows, n_exp):
    tok_n, top_n = expert_ids.shape
    flat_ids = expert_ids.reshape(tok_n * top_n)
    onehot = (flat_ids[:, None] == jnp.arange(n_exp)[None, :]).astype(jnp.int32)
    before = jnp.cumsum(onehot, axis=0) - onehot
    slot_idx = jnp.sum(before * onehot, axis=1)
    row_limit = jnp.sum(onehot * counts_row[None, :], axis=1)
    buf_pos = jnp.where(slot_idx < row_limit, flat_ids * cap_rows + slot_idx, -1)
    return buf_pos.reshape(tok_n, top_n)


def expert_ffn(rows_in, w_gate, w_up, w_down):
    act_a = jnp.einsum("erd,edf->erf", rows_in, w_gate, preferred_element_type=F32)
    act_b = jnp.einsum("erd,edf->erf", rows_in, w_up, preferred_element_type=F32)
    hidden = (jax.nn.silu(act_a) * act_b).astype(jnp.bfloat16)
    return jnp.einsum("erf,efd->erd", hidden, w_down, preferred_element_type=F32).astype(jnp.bfloat16)


def dense_step(group_size, tokens, expert_ids, gate_w, route_counts, w_gate, w_up, w_down):
    bf = jnp.bfloat16
    tok_n, top_n = expert_ids.shape
    n_exp = w_gate.shape[0] * group_size
    cap_rows, step = tok_n // 2, 4
    buf_pos = place_rows(expert_ids, route_counts[0], cap_rows, n_exp)
    rows = jnp.arange(n_exp * step)

    def exchange(x):
        return lax.all_to_all(x.reshape(group_size, step, -1), "ep", 0, 0, tiled=True)

    def batch(i, total):
        slot = jnp.where(buf_pos >= 0, buf_pos % cap_rows - i * step, -1)
        row = jnp.where((slot >= 0) & (slot < step), expert_ids * step + slot, -1)
        put = jnp.zeros((n_exp * step, tok_n), bf)
        for j in range(top_n):
            put = put + (rows[:, None] == row[None, :, j]).astype(bf)
        packed = jnp.dot(put, tokens, preferred_element_type=F32).astype(bf)
        y = expert_ffn(exchange(packed).reshape(1, n_exp * step, MODEL), w_gate, w_up, w_down)
        back = exchange(y).reshape(n_exp * step, MODEL)
        for j in range(top_n):
            got = (rows[None, :] == row[:, j][:, None]).astype(bf)
            total = total + gate_w[:, j][:, None] * jnp.dot(got, back, preferred_element_type=F32)
        return total

    return lax.fori_loop(0, cap_rows // step, batch, tokens.astype(F32)).astype(bf)


def chunk_of(wg, wu, wd, half, k):
    if k < 48:
        arr = wg if k < 24 else wu
        row, col = (k % 24) // 3, (k % 24) % 3
        start = half * 1024 + row * CH_R
    else:
        arr = wd
        row, col = (k - 48) // 8, (k - 48) % 8
        start = half * 384 + row * CH_R
    return arr.at[pl.ds(pl.multiple_of(start, CH_R), CH_R), pl.ds(col * CH_C, CH_C)]


def remote(src, dst, send, recv, dev):
    return pltpu.make_async_remote_copy(
        src_ref=src, dst_ref=dst, send_sem=send, recv_sem=recv, device_id={"ep": dev}, device_id_type=MESH
    )


def block_at(i, n):
    return pl.ds(i * n if isinstance(i, int) else pl.multiple_of(i * n, n), n)


def first(n):
    return pl.ds(0, n)


def others(ref):
    return ref.at[first(ref.shape[0] - 1)]


def plane_peer(grp, k):
    return ((grp // 4 + k // 4) % 4) * 4 + (grp % 4 + k % 4) % 4


def drain(ref, sem):
    pltpu.make_async_copy(ref, ref, sem).wait()


def ffn_rows(x, y, wg, wu, wd):
    def block(i, carry):
        at = block_at(i, 256)
        rows = x[at, :]
        a = jnp.dot(rows, wg[...], preferred_element_type=F32)
        b = jnp.dot(rows, wu[...], preferred_element_type=F32)
        h = (jax.nn.silu(a) * b).astype(jnp.bfloat16)
        y[at, :] = jnp.dot(h, wd[...], preferred_element_type=F32).astype(jnp.bfloat16)
        return carry

    lax.fori_loop(0, x.shape[0] // 256, block, 0)


def iota(shape, dim):
    return lax.broadcasted_iota(jnp.int32, shape, dim)


def ones_where(cond):
    return jnp.where(cond, 1.0, 0.0).astype(jnp.bfloat16)


def fdot(a, b):
    return jnp.dot(a.astype(jnp.bfloat16), b.astype(jnp.bfloat16), preferred_element_type=F32)


def main_kernel(tok, ids, gat, cnt, wg, wu, wd,
                rows_h, st, xr, cold_home, gh, gc, ok_all, info,
                own, inj, stage, recv, cg, cu, cd, toks, rows_c, arr, y_c, home_c, ret_c, hid,
                sl, gt, tab_all, cnt_all, hot_all, flags, hot_t, ok_t, ok_grp, rk, kc, sh, disp, kexp, pack, ght, gct,
                dma1, inj_r, ring_r):
    me = lax.axis_index("ep")
    grp, pos = me // GRP, me % GRP
    zz, yy = grp // 4, grp % 4
    core, xx = pos % 2, pos // 2
    other = 1 - core
    partner = grp * GRP + xx * 2 + other
    nbr = grp * GRP + ((xx + 1 + 2 * core) % 4) * 2 + core
    wg, wu, wd = wg.at[0], wu.at[0], wd.at[0]
    (own_sem, w0_sem, w1_sem, w2_sem, cnt_s, cnt_r, tab_s, tab_r, hot_s, hot_r, inj_s, a1_s, a1_r, b1_s, b1_r, p2_s, p2_r,
     xd_s, xd_r, ok_s, ok_r, xb_s, xb_r, pr_s, pr_r, oa_s, oa_r, ring_s, par_s, par_r, st_sem, loc_sem) = [dma1.at[i] for i in range(32)]

    def xdev(k):
        return grp * GRP + (pos + k) % GRP

    def pdev(k):
        return ((grp + k) % PLN) * GRP + pos

    for k in range(K):
        pltpu.make_async_copy(chunk_of(wg, wu, wd, core, k), own.at[k], own_sem).start()
    mine_at = block_at(grp, 64)
    pltpu.make_async_copy(tok, toks.at[mine_at], loc_sem).start()
    full = [pltpu.make_async_copy(s, d, q) for s, d, q in ((wg, cg, w0_sem), (wu, cu, w1_sem), (wd, cd, w2_sem))]

    sq = (128, 128)
    e_i = iota(sq, 0)
    named = jnp.zeros(sq, F32)
    gates = jnp.zeros(sq, F32)
    for j in range(8):
        hit_j = ids[j : j + 1, :] == e_i
        named = jnp.where(hit_j, 1.0, named)
        gates = jnp.where(hit_j, gat[j : j + 1, :], gates)
    l0, l1 = iota(sq, 0), iota(sq, 1)
    slot = fdot(named, ones_where(((l0 >> 6) == (l1 >> 6)) & (l0 < l1)))
    sl[...] = jnp.where((named > 0.5) & (slot < 32.0), slot, -1.0).reshape(PLN, *TILE)
    gt[...] = gates.reshape(PLN, *TILE)

    bar = pltpu.get_barrier_semaphore()
    for k in range(1, GRP):
        pl.semaphore_signal(bar, inc=1, device_id={"ep": xdev(k)}, device_id_type=MESH)
    for k in range(1, PLN):
        pl.semaphore_signal(bar, inc=1, device_id={"ep": pdev(k)}, device_id_type=MESH)
    pl.semaphore_wait(bar, GRP - 1 + PLN - 1)

    for k in range(1, GRP):
        remote(cnt, cnt_all.at[pos], cnt_s, cnt_r, xdev(k)).start()
    cnt_all[pos] = cnt[...]

    def half_at(z, y, h):
        return pl.ds(pl.multiple_of(((z % 4) * 4 + (y % 4)) * 64 + 32 * h, 32), 32)

    def plane_dev(z, y):
        return ((z % 4) * 4 + (y % 4)) * GRP + pos

    for k in (1, 3, 2):
        remote(tok.at[first(32)], toks.at[half_at(zz, yy, 0)], a1_s, a1_r, plane_dev(zz, yy + k)).start()
        remote(tok.at[pl.ds(32, 32)], toks.at[half_at(zz, yy, 1)], b1_s, b1_r, plane_dev(zz + k, yy)).start()
    for k in range(K):
        remote(chunk_of(wg, wu, wd, other, k), inj.at[k], inj_s, inj_r.at[k // INJ], partner).start()
    for k in range(1, PLN):
        remote(sl.at[(grp + k) % PLN], tab_all.at[grp], tab_s, tab_r, pdev(k)).start()
    tab_all[grp] = sl[grp]
    for cp in full:
        cp.start()

    drain(others(cnt_all), cnt_r)
    total = jnp.sum(cnt_all[...].astype(jnp.float32), axis=0)
    lane = iota(TILE, 1)
    key = total * 8.0 + (7 - (lane & 7)).astype(jnp.float32)
    key = jnp.where((lane >> 3) == grp, key, -1.0)
    best = jnp.max(key, **ACROSS)
    hit = jnp.where(key == best, 1.0, 0.0)
    mine = jnp.max(jnp.where(lane == me, hit, 0.0), **ACROSS)
    theirs = jnp.max(jnp.where(lane == partner, hit, 0.0), **ACROSS)
    flags[0] = jnp.broadcast_to(mine, TILE)
    flags[1] = jnp.broadcast_to(theirs, TILE)
    hot_p = jnp.max(jnp.where(lane == grp * 8 + iota(TILE, 0), hit, 0.0), **ACROSS)
    hot_t[...] = jnp.broadcast_to(hot_p, TILE)
    hx = jnp.sum(hit * ((lane & 7) >> 1).astype(jnp.float32), **ACROSS).astype(jnp.int32)
    sign = 1 - 2 * core
    hops = (sign * (xx - hx) + 8) & 3
    info[...] = jnp.where(iota(TILE, 0) == 0, D * hops, D * ((4 - hops) & 3))
    drain(own, own_sem)

    def flag(i):
        row = flags[i, 0:1, :]
        return jnp.concatenate([row, row], axis=1)

    def send(t, src, ring=True):
        if ring:
            remote(src, recv.at[t], ring_s, ring_r.at[t % N_SEM], nbr).start()
        remote(src, xr.at[t], par_s, par_r, partner).start()
        pltpu.make_async_copy(src, st.at[t], st_sem).start()

    def take(t):
        pltpu.make_async_copy(recv.at[t], recv.at[t], ring_r.at[t % N_SEM]).wait()

    def build(t, first):
        a = own[t].astype(jnp.float32)
        b = inj[t].astype(jnp.float32)
        if not first:
            b = jnp.where(flag(1) > 0.5, b, recv[t - D].astype(jnp.float32))
        stage[t] = jnp.where(flag(0) > 0.5, a, b).astype(jnp.bfloat16)

    def head(t):
        build(t, True)
        send(t - 1, stage.at[t - 1])

    def body(t):
        take(t - D)
        build(t, False)
        send(t - 1, stage.at[t - 1])

    def tail(t):
        take(t - D)
        send(t, recv.at[t - D])

    def last(t):
        take(t - D)
        send(t, recv.at[t - D], ring=False)

    at = [0]

    def ring(n, task=None):
        base = at[0]
        end = min(base + n, T)
        while at[0] < end:
            t = at[0]
            if t < K and t % INJ == 0:
                drain(inj.at[pl.ds(t, INJ)], inj_r.at[t // INJ])
            if t == K:
                send(K - 1, stage.at[K - 1])
            if t == 0:
                build(0, True)
                if task is not None:
                    task(0)
                at[0] = 1
                continue
            kind, stop = (head, D) if t < D else (body, (t // INJ + 1) * INJ) if t < K else (tail, N_RING) if t < N_RING else (last, T)
            stop = min(stop, end)

            def step(i, carry, kind=kind):
                kind(i)
                if task is not None:
                    task(i - base)
                return carry

            lax.fori_loop(t, stop, step, 0)
            at[0] = stop
        if task is not None:
            for i in range(end - base, n):
                task(i)

    ring(1)
    for k in range(1, PLN):
        remote(hot_t, hot_all.at[grp], hot_s, hot_r, pdev(k)).start()
    hot_all[grp] = hot_t[...]
    ring(3)
    pltpu.make_async_copy(tok, toks.at[mine_at], loc_sem).wait()
    drain(toks.at[first(96)], a1_r)
    drain(toks.at[first(96)], b1_r)
    for k in (2, 1, 3):
        for i in range(4):
            a_at, b_at = half_at(zz, yy + i, 0), half_at(zz + i, yy, 1)
            remote(toks.at[a_at], toks.at[a_at], p2_s, p2_r, plane_dev(zz + k, yy)).start()
            remote(toks.at[b_at], toks.at[b_at], p2_s, p2_r, plane_dev(zz, yy + k)).start()

    ring(3)
    drain(others(hot_all), hot_r)

    def gate_task(g):
        s, w, h = sl[g], gt[g], hot_all[g]
        s_h = jnp.sum(h * (s + 1.0), **DOWN) - 1.0
        w_h = jnp.sum(h * w, **DOWN)
        ght[block_at(g, 32), :] = jnp.where(iota((32, 128), 0).astype(jnp.float32) == s_h, w_h, 0.0)
        n = jnp.sum(jnp.where((s >= 0.0) & (lane < 64), 1.0 - h, 0.0), **ACROSS)
        off = jnp.zeros((1, 1), jnp.float32)
        acc = jnp.zeros((PITCH, 128), F32)
        r_i = iota((PITCH, 128), 0).astype(F32)
        for p in range(GRP):
            s_p = s[p : p + 1, :]
            use = (s_p >= 0.0) & (h[p : p + 1, :] < 0.5) & (s_p + off < CAP_B)
            r_p = jnp.where(use, s_p + off, -1.0)
            acc = acc + jnp.where(r_i == r_p, w[p : p + 1, :], 0.0)
            off = off + n[p : p + 1, :]
        gct[block_at(g, PITCH), :] = acc

    ring(16, gate_task)
    gh[...] = ght[...].T
    gc[...] = gct[...].T
    ring(1)

    drain(others(tab_all), tab_r)
    hot16 = jnp.concatenate([hot_t[:, 0:1], jnp.zeros((8, 1), jnp.float32)], axis=0)
    s8 = jnp.concatenate([jnp.where(lane < 64, tab_all[2 * i], tab_all[2 * i + 1]) for i in range(8)], axis=1)
    s16 = jnp.concatenate([s8, jnp.full((8, 1024), -1.0, jnp.float32)], axis=0)
    kept = s16 >= 0.0
    bm = ones_where((iota((1024, 128), 0) >> 6) == iota((1024, 128), 1))
    bt = ones_where((iota((128, 1024), 1) >> 6) == iota((128, 1024), 0))
    n_ps = fdot(jnp.where(kept, 1.0, 0.0), bm)
    offs = fdot(n_ps, ones_where(l0 < l1))
    off_l = fdot(jnp.minimum(offs, 255.0), bt)
    cold = kept & (hot16 < 0.5)
    rk[...] = jnp.where(cold, off_l + s16, -1.0)
    kc[...] = jnp.where(cold, 1.0, 0.0)
    sh[...] = jnp.broadcast_to(jnp.max(jnp.where(hot16 > 0.5, s16, -1.0), **DOWN), (8, 1024))
    ring(1)
    for p in range(GRP):
        at_p = block_at(p, CAP_C)
        disp[at_p, :] = ones_where(iota((CAP_C, 1024), 0).astype(jnp.float32) == rk[p : p + 1, :])
        kexp[at_p, :] = jnp.broadcast_to(kc[p : p + 1, :], (CAP_C, 1024)).astype(jnp.bfloat16)
        ring(1)
    n_e = lax.dot_general(bt, kexp[...], (((1,), (1,)), ((), ())), preferred_element_type=F32)
    most = jnp.max(jnp.sum(n_e, **DOWN), **ACROSS)
    row_most = jnp.max(jnp.sum(n_e, **ACROSS), **DOWN)
    fits = jnp.where((most <= CAP_C) & (row_most <= 32.0 * CAP_B), 1.0, 0.0)
    ok_t[0] = jnp.broadcast_to(fits, TILE)
    wide, tall = (256, 256), (512, 256)
    os_e = fdot(ones_where(l1 < l0), n_e)
    oc_e = fdot(n_e, ones_where(((iota(wide, 0) >> 5) < (iota(wide, 1) >> 5)) & ((iota(wide, 0) & 31) == 0)))
    e_row = ones_where((iota((512, 128), 0) >> 5) == iota((512, 128), 1))
    n_f = fdot(e_row, n_e)
    q_k = (iota(tall, 1) & 31).astype(jnp.float32) - fdot(e_row, jnp.minimum(os_e, 255.0))
    q_r = (iota(tall, 0) & 31).astype(jnp.float32) - fdot(e_row, jnp.minimum(oc_e, 255.0))
    pack[...] = ones_where((q_k == q_r) & (q_k >= 0.0) & (q_k < n_f))
    ring(RING_AG - at[0])

    drain(toks.at[first(768)], p2_r)

    def disp_task(c):
        cols = block_at(c, 256)
        block = jnp.dot(disp[...], toks[:, cols], preferred_element_type=F32).astype(jnp.bfloat16)
        rows_c[:, :, cols] = block.reshape(GRP, CAP_C, 256)

    ring(8, disp_task)
    arr[pos] = rows_c[pos]
    ok_grp[pos] = ok_t[0]

    def x_send(src, dst, s_sem, r_sem):
        def task(i):
            part = block_at(i, 8)
            for k in (1, 7, 2, 3, 4, 5, 6):
                remote(src.at[(pos + k) % GRP, part], dst.at[pos, part], s_sem, r_sem, xdev(k)).start()
        return task

    for k in range(1, GRP):
        remote(ok_t.at[0], ok_grp.at[pos], ok_s, ok_r, xdev(k)).start()
    ring(4, x_send(rows_c, arr, xd_s, xd_r))

    def hot_task(i):
        lanes = block_at(i, 128)
        slots = sh[0:1, lanes]
        r_i = iota((64, 128), 0)
        mine_rows = (r_i >> 5) == (iota((64, 128), 1) >> 6)
        pick = ones_where(mine_rows & ((r_i & 31).astype(jnp.float32) == slots))
        out = jnp.dot(pick, toks[block_at(i, 128), :], preferred_element_type=F32)
        rows_h[block_at(i, 64), :] = out.astype(jnp.bfloat16)

    ring(8, hot_task)
    ring(RING_X1)
    drain(others(arr), xd_r)
    drain(others(ok_grp), ok_r)
    ok_t[1] = jnp.min(ok_grp[...], axis=0)
    for cp in full:
        cp.wait()

    def up_task(c):
        cols = block_at(c, 256)
        x = arr[...].reshape(GRP * CAP_C, MODEL)
        a = jnp.dot(x, cg[:, cols], preferred_element_type=F32)
        b = jnp.dot(x, cu[:, cols], preferred_element_type=F32)
        hid[:, cols] = (jax.nn.silu(a) * b).astype(jnp.bfloat16)

    def down_task(c):
        cols = block_at(c, 512)
        y = jnp.dot(hid[...], cd[:, cols], preferred_element_type=F32).astype(jnp.bfloat16)
        y_c[:, :, cols] = y.reshape(GRP, CAP_C, 512)

    ring(3, up_task)
    ring(4, down_task)
    home_c[pos] = y_c[pos]
    ring(4, x_send(y_c, home_c, xb_s, xb_r))
    ring(RING_X2)
    drain(others(home_c), xb_r)

    def pack_task(c):
        cols = block_at(c, 512)
        block = jnp.dot(pack[...], home_c[:, :, cols].reshape(GRP * CAP_C, 512), preferred_element_type=F32)
        ret_c[:, :, cols] = block.astype(jnp.bfloat16).reshape(PLN, PITCH, 512)

    ring(4, pack_task)
    few = first(CAP_B)
    rest = pl.ds(CAP_B, PITCH - CAP_B)
    cold_home[:, rest, :] = jnp.zeros((PLN, PITCH - CAP_B, MODEL), jnp.bfloat16)
    cold_home[grp, few, :] = ret_c[grp, few, :]
    ok_all[grp] = ok_t[1]
    ring(1)
    for k in FAR:
        peer = plane_peer(grp, k)
        remote(ret_c.at[peer, few], cold_home.at[grp, few], pr_s, pr_r, peer * GRP + pos).start()
    for k in range(1, PLN):
        remote(ok_t.at[1], ok_all.at[grp], oa_s, oa_r, pdev(k)).start()
    ring(T)

    drain(others(cnt_all), cnt_s)
    drain(others(tab_all), tab_s)
    drain(others(hot_all), hot_s)
    drain(toks.at[first(96)], a1_s)
    drain(toks.at[first(96)], b1_s)
    drain(toks.at[first(768)], p2_s)
    drain(others(ok_grp), ok_s)
    drain(others(arr), xd_s)
    drain(others(home_c), xb_s)
    drain(inj, inj_s)
    drain(recv, ring_s)
    drain(st, st_sem)
    drain(xr, par_s)
    drain(xr, par_r)
    drain(others(ok_all), oa_s)
    drain(others(ok_all), oa_r)
    drain(cold_home.at[first(PLN - 1), few], pr_s)
    drain(cold_home.at[first(PLN - 1), few], pr_r)


def main_call(tokens, ids_t, gat_t, cnt_t, w_gate, w_up, w_down):
    dma = pltpu.SemaphoreType.DMA
    bf, f32 = jnp.bfloat16, jnp.float32
    vm, an = pl.BlockSpec(memory_space=VMEM), pl.BlockSpec(memory_space=ANY)
    chunks = lambda n: VMEM((n, CH_R, CH_C), bf)
    tile = lambda *n: VMEM((*n, *TILE), f32)
    rows = VMEM((GRP, CAP_C, MODEL), bf)
    out = jax.ShapeDtypeStruct
    return pl.pallas_call(
        main_kernel,
        out_shape=(
            out((512, MODEL), bf), out((T, CH_R, CH_C), bf), out((T, CH_R, CH_C), bf), out((PLN, PITCH, MODEL), bf),
            out((128, 512), f32), out((128, 512), f32), out((PLN, *TILE), f32), out(TILE, jnp.int32),
        ),
        in_specs=[vm, vm, vm, vm, an, an, an],
        out_specs=(vm, an, an, vm, vm, vm, vm, vm),
        scratch_shapes=[
            chunks(K), chunks(K), chunks(K), chunks(N_RING),
            VMEM((MODEL, FFN), bf), VMEM((MODEL, FFN), bf), VMEM((FFN, MODEL), bf),
            VMEM((1024, MODEL), bf), rows, rows, rows, rows, VMEM((PLN, PITCH, MODEL), bf), VMEM((GRP * CAP_C, FFN), bf),
            tile(PLN), tile(PLN), tile(PLN), VMEM((GRP, *TILE), jnp.int32), tile(PLN), tile(2), tile(), tile(2), tile(GRP),
            VMEM((16, 1024), f32), VMEM((16, 1024), f32), VMEM((8, 1024), f32), VMEM((256, 1024), bf), VMEM((256, 1024), bf),
            VMEM((512, 256), bf), VMEM((512, 128), f32), VMEM((512, 128), f32),
            dma((32,)), dma((K // INJ,)), dma((N_SEM,)),
        ],
        compiler_params=pltpu.CompilerParams(collective_id=0, **EFFECTS, vmem_limit_bytes=60 * MIB),
    )(tokens, ids_t, gat_t, cnt_t, w_gate, w_up, w_down)


def hot_kernel(info, st, xr, wg, wu, wd, x, y, hg, hu, hd, sems):
    core = lax.axis_index("ep") % 2
    first, second = info[0, 0], info[1, 0]
    for k in range(K):
        sem = sems.at[k // 24]
        pltpu.make_async_copy(st.at[first + k], chunk_of(hg, hu, hd, core, k), sem).start()
        pltpu.make_async_copy(xr.at[second + k], chunk_of(hg, hu, hd, 1 - core, k), sem).start()
    for i, (s, d) in enumerate(((wg.at[0], hg), (wu.at[0], hu), (wd.at[0], hd))):
        pltpu.make_async_copy(s, d, sems.at[i]).wait()
    ffn_rows(x, y, hg, hu, hd)


def hot_call(info, st, xr, w_gate, w_up, w_down, x):
    bf = jnp.bfloat16
    vm, an = pl.BlockSpec(memory_space=VMEM), pl.BlockSpec(memory_space=ANY)
    return pl.pallas_call(
        hot_kernel,
        out_shape=jax.ShapeDtypeStruct(x.shape, bf),
        in_specs=[pl.BlockSpec(memory_space=pltpu.SMEM), an, an, an, an, an, vm],
        out_specs=vm,
        scratch_shapes=[VMEM((MODEL, FFN), bf), VMEM((MODEL, FFN), bf), VMEM((FFN, MODEL), bf), pltpu.SemaphoreType.DMA((3,))],
        compiler_params=pltpu.CompilerParams(vmem_limit_bytes=40 * MIB),
    )(info, st, xr, w_gate, w_up, w_down, x)


def final_kernel(y, tok, gh, gc, cold, out, home, acc, row_s, row_r):
    me = lax.axis_index("ep")
    grp, pos = me // GRP, me % GRP
    bar = pltpu.get_barrier_semaphore()
    for k in range(1, PLN):
        pl.semaphore_signal(bar, inc=1, device_id={"ep": ((grp + k) % PLN) * GRP + pos}, device_id_type=MESH)
    pl.semaphore_wait(bar, PLN - 1)
    for k in FAR:
        peer = plane_peer(grp, k)
        remote(y.at[peer], home.at[grp], row_s, row_r, peer * GRP + pos).start()
    home[grp] = y[grp]

    def pieces(g):
        g1 = g.astype(jnp.bfloat16)
        r1 = g - g1.astype(jnp.float32)
        g2 = r1.astype(jnp.bfloat16)
        g3 = (r1 - g2.astype(jnp.float32)).astype(jnp.bfloat16)
        return jnp.concatenate([g1, g2, g3], axis=0)

    def add(g, vals):
        parts = jnp.dot(g, vals, preferred_element_type=F32)
        return parts[:64] + (parts[64:128] + parts[128:])

    w_c, w_h = pieces(gc[0:64, :]), pieces(gh[0:64, :])
    for c in range(4):
        cols = block_at(c, 512)
        vals = cold[:, :, cols].reshape(512, 512)
        acc[:, cols] = tok[:, cols].astype(jnp.float32) + add(w_c, vals)
    drain(others(home), row_r)
    for c in range(4):
        cols = block_at(c, 512)
        vals = home[:, :, cols].reshape(512, 512)
        out[:, cols] = (acc[:, cols] + add(w_h, vals)).astype(jnp.bfloat16)
    drain(others(home), row_s)


def final_call(y, tokens, gh, gc, cold):
    bf = jnp.bfloat16
    vm = pl.BlockSpec(memory_space=VMEM)
    return pl.pallas_call(
        final_kernel,
        out_shape=jax.ShapeDtypeStruct((64, MODEL), bf),
        in_specs=[vm] * 5,
        out_specs=vm,
        scratch_shapes=[VMEM((PLN, 32, MODEL), bf), VMEM((64, MODEL), jnp.float32), pltpu.SemaphoreType.DMA, pltpu.SemaphoreType.DMA],
        compiler_params=pltpu.CompilerParams(collective_id=1, **EFFECTS, vmem_limit_bytes=40 * MIB),
    )(y, tokens, gh, gc, cold)


def sparse_step(tokens, expert_ids, gate_w, route_counts, w_gate, w_up, w_down):
    ids_t = jnp.concatenate([expert_ids.T, expert_ids.T], axis=1)
    gat_t = jnp.concatenate([gate_w.T, gate_w.T], axis=1)
    cnt_t = jnp.broadcast_to(route_counts, TILE)
    rows_h, st, xr, cold, gh, gc, ok_all, info = main_call(tokens, ids_t, gat_t, cnt_t, w_gate, w_up, w_down)
    y_h = hot_call(info, st, xr, w_gate, w_up, w_down, rows_h)
    out = final_call(y_h.reshape(PLN, 32, MODEL), tokens, gh, gc, cold)
    return out, jnp.min(ok_all) > 0.5


def solution(mesh):
    group_size = mesh.shape["ep"]
    row_spec = P(("dp", "ep"))

    def local_step(*args):
        fast, ok = sparse_step(*args)
        return lax.cond(ok, lambda: fast, lambda: dense_step(group_size, *args))

    return jax.shard_map(
        local_step,
        mesh=mesh,
        in_specs=(row_spec, row_spec, row_spec, row_spec, P("ep"), P("ep"), P("ep")),
        out_specs=row_spec,
        check_vma=False,
    )
```

```python
import functools

import jax
import jax.numpy as jnp
from jax import lax
from jax.experimental import pallas as pl
from jax.experimental.pallas import tpu as pltpu
from jax.sharding import PartitionSpec as P

MESH = pl.DeviceIdType.MESH
VMEM = pltpu.VMEM
ANY = pl.ANY
F32 = jnp.float32
MODEL, FFN, TILE, MIB = 2048, 768, (8, 128), 2**20
DOWN, ACROSS = dict(axis=0, keepdims=True), dict(axis=1, keepdims=True)
EFFECTS = dict(has_side_effects=True)
GRP = 8
PLN = 16
CAP_C = 32
CH_R, CH_C = 128, 256
K = 72
D = 7
T = K + 3 * D
N_RING = K + 2 * D
N_SEM = 32
INJ = 12
PITCH = 32
SELF = 10
CAP_B = 24
RING_AG = 44
RING_X1, RING_X2 = 8, 12
FAR = (10, 6, 14, 9, 11, 2, 8, 5, 7, 13, 15, 1, 3, 4, 12)


def place_rows(expert_ids, counts_row, cap_rows, n_exp):
    tok_n, top_n = expert_ids.shape
    flat_ids = expert_ids.reshape(tok_n * top_n)
    onehot = (flat_ids[:, None] == jnp.arange(n_exp)[None, :]).astype(jnp.int32)
    before = jnp.cumsum(onehot, axis=0) - onehot
    slot_idx = jnp.sum(before * onehot, axis=1)
    row_limit = jnp.sum(onehot * counts_row[None, :], axis=1)
    buf_pos = jnp.where(slot_idx < row_limit, flat_ids * cap_rows + slot_idx, -1)
    return buf_pos.reshape(tok_n, top_n)


def expert_ffn(rows_in, w_gate, w_up, w_down):
    act_a = jnp.einsum("erd,edf->erf", rows_in, w_gate, preferred_element_type=F32)
    act_b = jnp.einsum("erd,edf->erf", rows_in, w_up, preferred_element_type=F32)
    hidden = (jax.nn.silu(act_a) * act_b).astype(jnp.bfloat16)
    return jnp.einsum("erf,efd->erd", hidden, w_down, preferred_element_type=F32).astype(jnp.bfloat16)


def dense_step(group_size, tokens, expert_ids, gate_w, route_counts, w_gate, w_up, w_down):
    bf = jnp.bfloat16
    tok_n, top_n = expert_ids.shape
    n_exp = w_gate.shape[0] * group_size
    cap_rows, step = tok_n // 2, 4
    buf_pos = place_rows(expert_ids, route_counts[0], cap_rows, n_exp)
    rows = jnp.arange(n_exp * step)

    def exchange(x):
        return lax.all_to_all(x.reshape(group_size, step, -1), "ep", 0, 0, tiled=True)

    def batch(i, total):
        slot = jnp.where(buf_pos >= 0, buf_pos % cap_rows - i * step, -1)
        row = jnp.where((slot >= 0) & (slot < step), expert_ids * step + slot, -1)
        put = jnp.zeros((n_exp * step, tok_n), bf)
        for j in range(top_n):
            put = put + (rows[:, None] == row[None, :, j]).astype(bf)
        packed = jnp.dot(put, tokens, preferred_element_type=F32).astype(bf)
        y = expert_ffn(exchange(packed).reshape(1, n_exp * step, MODEL), w_gate, w_up, w_down)
        back = exchange(y).reshape(n_exp * step, MODEL)
        for j in range(top_n):
            got = (rows[None, :] == row[:, j][:, None]).astype(bf)
            total = total + gate_w[:, j][:, None] * jnp.dot(got, back, preferred_element_type=F32)
        return total

    return lax.fori_loop(0, cap_rows // step, batch, tokens.astype(F32)).astype(bf)


def chunk_of(wg, wu, wd, half, k):
    if k < 48:
        arr = wg if k < 24 else wu
        row, col = (k % 24) // 3, (k % 24) % 3
        start = half * 1024 + row * CH_R
    else:
        arr = wd
        row, col = (k - 48) // 8, (k - 48) % 8
        start = half * 384 + row * CH_R
    return arr.at[pl.ds(pl.multiple_of(start, CH_R), CH_R), pl.ds(col * CH_C, CH_C)]


def remote(src, dst, send, recv, dev):
    return pltpu.make_async_remote_copy(
        src_ref=src, dst_ref=dst, send_sem=send, recv_sem=recv, device_id={"ep": dev}, device_id_type=MESH
    )


def block_at(i, n):
    return pl.ds(i * n if isinstance(i, int) else pl.multiple_of(i * n, n), n)


def first(n):
    return pl.ds(0, n)


def others(ref):
    return ref.at[first(ref.shape[0] - 1)]


def plane_peer(grp, k):
    return ((grp // 4 + k // 4) % 4) * 4 + (grp % 4 + k % 4) % 4


def drain(ref, sem):
    pltpu.make_async_copy(ref, ref, sem).wait()


def iota(shape, dim):
    return lax.broadcasted_iota(jnp.int32, shape, dim)


def ones_where(cond):
    return jnp.where(cond, 1.0, 0.0).astype(jnp.bfloat16)


def fdot(a, b):
    return jnp.dot(a.astype(jnp.bfloat16), b.astype(jnp.bfloat16), preferred_element_type=F32)


def main_kernel(tok, ids, gat, cnt, wg, wu, wd, out, ok_all,
                inj, stage, recv, xr, cg, cu, cd, toks, rows_c, arr, y_c, home_c, ret_c, cold_home, rows_h, y_h, home_h, hid, acc_ref,
                sl, gt, tab_all, cnt_me, cnt_all, hot_all, flags, hot_t, ok_t, ok_grp, rk, kc, disp, kexp, pack, ght, gct, gh, gc,
                dma1, inj_r, ring_r):
    me = lax.axis_index("ep")
    grp, pos = me // GRP, me % GRP
    zz, yy = grp // 4, grp % 4
    core, xx = pos % 2, pos // 2
    other = 1 - core
    partner = grp * GRP + xx * 2 + other
    nbr = grp * GRP + ((xx + 1 + 2 * core) % 4) * 2 + core
    wg, wu, wd = wg.at[0], wu.at[0], wd.at[0]
    (hh_s, hh_r, w0_sem, w1_sem, w2_sem, cnt_s, cnt_r, tab_s, tab_r, hot_s, hot_r, inj_s, a1_s, a1_r, b1_s, b1_r, p2_s, p2_r,
     xd_s, xd_r, ok_s, ok_r, xb_s, xb_r, pr_s, pr_r, oa_s, oa_r, ring_s, par_s, par_r, loc_sem) = [dma1.at[i] for i in range(32)]

    def far_peer(i):
        z_off, y_off = (i // 4 + 2) % 4, (i % 4 + 2) % 4
        return ((zz + z_off) % 4) * 4 + (yy + y_off) % 4

    def xdev(k):
        return grp * GRP + (pos + k) % GRP

    def pdev(k):
        return ((grp + k) % PLN) * GRP + pos

    mine_at = block_at(grp, 64)
    pltpu.make_async_copy(tok, toks.at[mine_at], loc_sem).start()
    full = [pltpu.make_async_copy(s, d, q) for s, d, q in ((wg, cg, w0_sem), (wu, cu, w1_sem), (wd, cd, w2_sem))]
    for cp in full:
        cp.start()
    cnt_me[...] = jnp.broadcast_to(cnt[...], TILE)

    sq = (128, 128)
    e_i = iota(sq, 0)
    named = jnp.zeros(sq, F32)
    gates = jnp.zeros(sq, F32)
    ids2 = jnp.concatenate([ids[...], ids[...]], axis=1)
    gat2 = jnp.concatenate([gat[...], gat[...]], axis=1)
    for j in range(8):
        hit_j = ids2[j : j + 1, :] == e_i
        named = jnp.where(hit_j, 1.0, named)
        gates = jnp.where(hit_j, gat2[j : j + 1, :], gates)
    l0, l1 = iota(sq, 0), iota(sq, 1)
    slot = fdot(named, ones_where(((l0 >> 6) == (l1 >> 6)) & (l0 < l1)))
    sl[...] = jnp.where((named > 0.5) & (slot < 32.0), slot, -1.0).reshape(PLN, *TILE)
    gt[...] = gates.reshape(PLN, *TILE)

    bar = pltpu.get_barrier_semaphore()
    for k in range(1, GRP):
        pl.semaphore_signal(bar, inc=1, device_id={"ep": xdev(k)}, device_id_type=MESH)
    for k in range(1, PLN):
        pl.semaphore_signal(bar, inc=1, device_id={"ep": pdev(k)}, device_id_type=MESH)
    pl.semaphore_wait(bar, GRP - 1 + PLN - 1)

    for k in range(1, GRP):
        remote(cnt_me, cnt_all.at[pos], cnt_s, cnt_r, xdev(k)).start()
    cnt_all[pos] = cnt_me[...]

    def half_at(z, y, h):
        return pl.ds(pl.multiple_of(((z % 4) * 4 + (y % 4)) * 64 + 32 * h, 32), 32)

    def plane_dev(z, y):
        return ((z % 4) * 4 + (y % 4)) * GRP + pos

    for k in (1, 3, 2):
        remote(tok.at[first(32)], toks.at[half_at(zz, yy, 0)], a1_s, a1_r, plane_dev(zz, yy + k)).start()
        remote(tok.at[pl.ds(32, 32)], toks.at[half_at(zz, yy, 1)], b1_s, b1_r, plane_dev(zz + k, yy)).start()
    for k in (1, 3, 2):
        remote(tok.at[first(32)], toks.at[half_at(zz, yy, 0)], p2_s, p2_r, plane_dev(zz + k, yy)).start()
        remote(tok.at[pl.ds(32, 32)], toks.at[half_at(zz, yy, 1)], p2_s, p2_r, plane_dev(zz, yy + k)).start()
    for k in range(K):
        remote(chunk_of(wg, wu, wd, other, k), inj.at[k], inj_s, inj_r.at[k // INJ], partner).start()
    for k in range(1, PLN):
        remote(sl.at[(grp + k) % PLN], tab_all.at[grp], tab_s, tab_r, pdev(k)).start()
    tab_all[grp] = sl[grp]

    drain(others(cnt_all), cnt_r)
    total = jnp.sum(cnt_all[...].astype(jnp.float32), axis=0)
    lane = iota(TILE, 1)
    key = total * 8.0 + (7 - (lane & 7)).astype(jnp.float32)
    key = jnp.where((lane >> 3) == grp, key, -1.0)
    best = jnp.max(key, **ACROSS)
    hit = jnp.where(key == best, 1.0, 0.0)
    mine = jnp.max(jnp.where(lane == me, hit, 0.0), **ACROSS)
    theirs = jnp.max(jnp.where(lane == partner, hit, 0.0), **ACROSS)
    flags[0] = jnp.broadcast_to(mine, TILE)
    flags[1] = jnp.broadcast_to(theirs, TILE)
    hot_p = jnp.max(jnp.where(lane == grp * 8 + iota(TILE, 0), hit, 0.0), **ACROSS)
    hot_t[...] = jnp.broadcast_to(hot_p, TILE)
    hx = jnp.sum(hit * ((lane & 7) >> 1).astype(jnp.float32), **ACROSS).astype(jnp.int32)
    sign = 1 - 2 * core
    hops = (sign * (xx - hx) + 8) & 3
    hops = jnp.max(hops.astype(F32)).astype(jnp.int32)
    full[0].wait()

    def flag(i):
        row = flags[i, 0:1, :]
        return jnp.concatenate([row, row], axis=1)

    def send(t, src, ring=True):
        if ring:
            remote(src, recv.at[t], ring_s, ring_r.at[t % N_SEM], nbr).start()
        remote(src, xr.at[t], par_s, par_r, partner).start()

    def take(t):
        pltpu.make_async_copy(recv.at[t], recv.at[t], ring_r.at[t % N_SEM]).wait()

    def own_chunk(arr_i, t):
        if arr_i < 2:
            k = t - 24 * arr_i
            row, col = core * 1024 + (k // 3) * CH_R, (k % 3) * CH_C
        else:
            k = t - 48
            row, col = core * 384 + (k // 8) * CH_R, (k % 8) * CH_C
        return (cg, cu, cd)[arr_i][pl.ds(pl.multiple_of(row, CH_R), CH_R), pl.ds(pl.multiple_of(col, CH_C), CH_C)]

    def build(t, first, arr_i):
        a = own_chunk(arr_i, t).astype(jnp.float32)
        b = inj[t].astype(jnp.float32)
        if not first:
            b = jnp.where(flag(1) > 0.5, b, recv[t - D].astype(jnp.float32))
        stage[t] = jnp.where(flag(0) > 0.5, a, b).astype(jnp.bfloat16)

    def head(t, arr_i):
        build(t, True, 0)
        send(t - 1, stage.at[t - 1])

    def body(t, arr_i):
        take(t - D)
        build(t, False, arr_i)
        send(t - 1, stage.at[t - 1])

    def tail(t, arr_i):
        take(t - D)
        stage[t] = recv[t - D]
        send(t, recv.at[t - D])

    def last(t, arr_i):
        take(t - D)
        stage[t] = recv[t - D]
        send(t, recv.at[t - D], ring=False)

    at = [0]

    def ring(n, task=None):
        base = at[0]
        end = min(base + n, T)
        while at[0] < end:
            t = at[0]
            if t in (24, 48):
                full[t // 24].wait()
            if t < K and t % INJ == 0:
                drain(inj.at[pl.ds(t, INJ)], inj_r.at[t // INJ])
            if t == K:
                send(K - 1, stage.at[K - 1])
            if t == 0:
                build(0, True, 0)
                if task is not None:
                    task(0)
                at[0] = 1
                continue
            kind, stop = (head, D) if t < D else (body, (t // INJ + 1) * INJ) if t < K else (tail, N_RING) if t < N_RING else (last, T)
            stop = min(stop, end)

            def step(i, carry, kind=kind, arr_i=t // 24):
                kind(i, arr_i)
                if task is not None:
                    task(i - base)
                return carry

            lax.fori_loop(t, stop, step, 0)
            at[0] = stop
        if task is not None:
            for i in range(end - base, n):
                task(i)

    ring(1)
    for k in range(1, PLN):
        remote(hot_t, hot_all.at[grp], hot_s, hot_r, pdev(k)).start()
    hot_all[grp] = hot_t[...]
    ring(3)
    pltpu.make_async_copy(tok, toks.at[mine_at], loc_sem).wait()
    drain(toks.at[first(96)], a1_r)
    drain(toks.at[first(96)], b1_r)
    for k in (1, 3, 2):
        for i in range(1, 4):
            a_at, b_at = half_at(zz, yy + i, 0), half_at(zz + i, yy, 1)
            remote(toks.at[a_at], toks.at[a_at], p2_s, p2_r, plane_dev(zz + k, yy)).start()
            remote(toks.at[b_at], toks.at[b_at], p2_s, p2_r, plane_dev(zz, yy + k)).start()

    ring(3)
    drain(others(hot_all), hot_r)

    def gate_task(g):
        s, w, h = sl[g], gt[g], hot_all[g]
        s_h = jnp.sum(h * (s + 1.0), **DOWN) - 1.0
        w_h = jnp.sum(h * w, **DOWN)
        ght[block_at(g, 32), :] = jnp.where(iota((32, 128), 0).astype(jnp.float32) == s_h, w_h, 0.0)
        n = jnp.sum(jnp.where((s >= 0.0) & (lane < 64), 1.0 - h, 0.0), **ACROSS)
        off = jnp.zeros((1, 1), jnp.float32)
        acc = jnp.zeros((PITCH, 128), F32)
        r_i = iota((PITCH, 128), 0).astype(F32)
        for p in range(GRP):
            s_p = s[p : p + 1, :]
            use = (s_p >= 0.0) & (h[p : p + 1, :] < 0.5) & (s_p + off < CAP_B)
            r_p = jnp.where(use, s_p + off, -1.0)
            acc = acc + jnp.where(r_i == r_p, w[p : p + 1, :], 0.0)
            off = off + n[p : p + 1, :]
        gct[block_at(g, PITCH), :] = acc

    ring(16, gate_task)
    gh[...] = ght[...].T
    gc[...] = gct[...].T
    ring(1)

    drain(others(tab_all), tab_r)
    hot16 = jnp.concatenate([hot_t[:, 0:1], jnp.zeros((8, 1), jnp.float32)], axis=0)
    s8 = jnp.concatenate([jnp.where(lane < 64, tab_all[2 * i], tab_all[2 * i + 1]) for i in range(8)], axis=1)
    s16 = jnp.concatenate([s8, jnp.full((8, 1024), -1.0, jnp.float32)], axis=0)
    kept = s16 >= 0.0
    bm = ones_where((iota((1024, 128), 0) >> 6) == iota((1024, 128), 1))
    bt = ones_where((iota((128, 1024), 1) >> 6) == iota((128, 1024), 0))
    n_ps = fdot(jnp.where(kept, 1.0, 0.0), bm)
    offs = fdot(n_ps, ones_where(l0 < l1))
    off_l = fdot(jnp.minimum(offs, 255.0), bt)
    cold = kept & (hot16 < 0.5)
    rk[...] = jnp.where(cold, off_l + s16, -1.0)
    kc[...] = jnp.where(cold, 1.0, 0.0)
    ring(1)
    for p in range(GRP):
        at_p = block_at(p, CAP_C)
        disp[at_p, :] = ones_where(iota((CAP_C, 1024), 0).astype(jnp.float32) == rk[p : p + 1, :])
        kexp[at_p, :] = jnp.broadcast_to(kc[p : p + 1, :], (CAP_C, 1024)).astype(jnp.bfloat16)
        ring(1)
    n_e = lax.dot_general(bt, kexp[...], (((1,), (1,)), ((), ())), preferred_element_type=F32)
    most = jnp.max(jnp.sum(n_e, **DOWN), **ACROSS)
    row_most = jnp.max(jnp.sum(n_e, **ACROSS), **DOWN)
    fits = jnp.where((most <= CAP_C) & (row_most <= 32.0 * CAP_B), 1.0, 0.0)
    ok_t[0] = jnp.broadcast_to(fits, TILE)
    wide, tall = (256, 256), (512, 256)
    os_e = fdot(ones_where(l1 < l0), n_e)
    oc_e = fdot(n_e, ones_where(((iota(wide, 0) >> 5) < (iota(wide, 1) >> 5)) & ((iota(wide, 0) & 31) == 0)))
    e_row = ones_where((iota((512, 128), 0) >> 5) == iota((512, 128), 1))
    n_f = fdot(e_row, n_e)
    q_k = (iota(tall, 1) & 31).astype(jnp.float32) - fdot(e_row, jnp.minimum(os_e, 255.0))
    q_r = (iota(tall, 0) & 31).astype(jnp.float32) - fdot(e_row, jnp.minimum(oc_e, 255.0))
    pack[...] = ones_where((q_k == q_r) & (q_k >= 0.0) & (q_k < n_f))
    ring(RING_AG - at[0])

    drain(toks.at[first(768)], p2_r)

    def disp_task(c):
        cols = block_at(c, 256)
        block = jnp.dot(disp[...], toks[:, cols], preferred_element_type=F32).astype(jnp.bfloat16)
        rows_c[:, :, cols] = block.reshape(GRP, CAP_C, 256)

    ring(8, disp_task)
    arr[pos] = rows_c[pos]
    ok_grp[pos] = ok_t[0]

    def x_send(src, dst, s_sem, r_sem):
        def task(i):
            part = block_at(i, 8)
            for k in (1, 7, 2, 3, 4, 5, 6):
                remote(src.at[(pos + k) % GRP, part], dst.at[pos, part], s_sem, r_sem, xdev(k)).start()
        return task

    for k in range(1, GRP):
        remote(ok_t.at[0], ok_grp.at[pos], ok_s, ok_r, xdev(k)).start()
    ring(4, x_send(rows_c, arr, xd_s, xd_r))

    def hot_task(i):
        for half in range(2):
            peer = far_peer(2 * i + half)
            slots = jnp.max(jnp.where(hot_t[...] > 0.5, tab_all[peer], -1.0), **DOWN)
            pick = ones_where(iota((32, 64), 0).astype(F32) == slots[:, 0:64])
            out_rows = jnp.dot(pick, toks[block_at(peer, 64), :], preferred_element_type=F32)
            rows_h[block_at(2 * i + half, 32), :] = out_rows.astype(jnp.bfloat16)

    ring(8, hot_task)
    ring(RING_X1)
    drain(others(arr), xd_r)
    drain(others(ok_grp), ok_r)
    ok_t[1] = jnp.min(ok_grp[...], axis=0)
    def up_task(c):
        cols = block_at(c, 256)
        x = arr[...].reshape(GRP * CAP_C, MODEL)
        a = jnp.dot(x, cg[:, cols], preferred_element_type=F32)
        b = jnp.dot(x, cu[:, cols], preferred_element_type=F32)
        hid[:, cols] = (jax.nn.silu(a) * b).astype(jnp.bfloat16)

    def down_task(c):
        cols = block_at(c, 512)
        y = jnp.dot(hid[...], cd[:, cols], preferred_element_type=F32).astype(jnp.bfloat16)
        y_c[:, :, cols] = y.reshape(GRP, CAP_C, 512)

    ring(3, up_task)
    ring(4, down_task)
    home_c[pos] = y_c[pos]
    ring(4, x_send(y_c, home_c, xb_s, xb_r))
    ring(RING_X2)
    drain(others(home_c), xb_r)

    def pack_task(c):
        cols = block_at(c, 512)
        block = jnp.dot(pack[...], home_c[:, :, cols].reshape(GRP * CAP_C, 512), preferred_element_type=F32)
        ret_c[:, :, cols] = block.astype(jnp.bfloat16).reshape(PLN, PITCH, 512)

    ring(4, pack_task)
    few = first(CAP_B)
    rest = pl.ds(CAP_B, PITCH - CAP_B)
    cold_home[:, rest, :] = jnp.zeros((PLN, PITCH - CAP_B, MODEL), jnp.bfloat16)
    cold_home[grp, few, :] = ret_c[grp, few, :]
    ok_all[grp] = ok_t[1]
    ring(1)
    for k in FAR:
        peer = plane_peer(grp, k)
        remote(ret_c.at[peer, few], cold_home.at[grp, few], pr_s, pr_r, peer * GRP + pos).start()
    for k in range(1, PLN):
        remote(ok_t.at[1], ok_all.at[grp], oa_s, oa_r, pdev(k)).start()
    ring(T)

    drain(xr, par_r)
    near, cross = D * (hops & 3), D * ((4 - hops) & 3)

    def gather_up(arr, base):
        def copy(i, carry):
            cols = pl.ds(pl.multiple_of((i % 3) * CH_C, CH_C), CH_C)
            for src, off, half in ((stage, near, core), (xr, cross, other)):
                rows = pl.ds(pl.multiple_of(half * 1024 + (i // 3) * CH_R, CH_R), CH_R)
                arr[rows, cols] = src[off + base + i]
            return carry

        lax.fori_loop(0, 24, copy, 0)

    def gather_down(i, carry):
        cols = pl.ds(pl.multiple_of((i % 8) * CH_C, CH_C), CH_C)
        for src, off, half in ((stage, near, core), (xr, cross, other)):
            rows = pl.ds(pl.multiple_of(half * 384 + (i // 8) * CH_R, CH_R), CH_R)
            cd[rows, cols] = src[off + 48 + i]
        return carry

    gather_up(cg, 0)
    gather_up(cu, 24)
    lax.fori_loop(0, 24, gather_down, 0)

    for blk in range(2):
        x = rows_h[block_at(blk, 256), :]
        for c in range(3):
            cols = block_at(c, 256)
            a = jnp.dot(x, cg[:, cols], preferred_element_type=F32)
            b = jnp.dot(x, cu[:, cols], preferred_element_type=F32)
            hid[:, cols] = (jax.nn.silu(a) * b).astype(jnp.bfloat16)
        for c in range(4):
            cols = block_at(c, 512)
            y = jnp.dot(hid[...], cd[:, cols], preferred_element_type=F32).astype(jnp.bfloat16)
            y_h[block_at(blk, 8), :, cols] = y.reshape(8, 32, 512)
        for i in range(8 * blk, 8 * blk + 8):
            if i != SELF:
                peer = far_peer(i)
                remote(y_h.at[i], home_h.at[grp], hh_s, hh_r, peer * GRP + pos).start()
    home_h[grp] = y_h[SELF]

    def pieces(g):
        g1 = g.astype(jnp.bfloat16)
        r1 = g - g1.astype(F32)
        g2 = r1.astype(jnp.bfloat16)
        g3 = (r1 - g2.astype(F32)).astype(jnp.bfloat16)
        return jnp.concatenate([g1, g2, g3], axis=0)

    def add(g, vals):
        parts = jnp.dot(g, vals, preferred_element_type=F32)
        return parts[:64] + (parts[64:128] + parts[128:])

    w_c, w_h = pieces(gc[0:64, :]), pieces(gh[0:64, :])
    drain(cold_home.at[first(PLN - 1), few], pr_r)
    for c in range(4):
        cols = block_at(c, 512)
        vals = cold_home[:, :, cols].reshape(512, 512)
        acc_ref[:, cols] = tok[:, cols].astype(F32) + add(w_c, vals)
    drain(others(home_h), hh_r)
    for c in range(4):
        cols = block_at(c, 512)
        vals = home_h[:, :, cols].reshape(512, 512)
        out[:, cols] = (acc_ref[:, cols] + add(w_h, vals)).astype(jnp.bfloat16)

    drain(others(cnt_all), cnt_s)
    drain(others(tab_all), tab_s)
    drain(others(hot_all), hot_s)
    drain(toks.at[first(96)], a1_s)
    drain(toks.at[first(96)], b1_s)
    drain(toks.at[first(768)], p2_s)
    drain(others(ok_grp), ok_s)
    drain(others(arr), xd_s)
    drain(others(home_c), xb_s)
    drain(inj, inj_s)
    drain(recv, ring_s)
    drain(xr, par_s)
    drain(others(home_h), hh_s)
    drain(others(ok_all), oa_s)
    drain(others(ok_all), oa_r)
    drain(cold_home.at[first(PLN - 1), few], pr_s)


def main_call(tokens, ids_t, gat_t, counts, w_gate, w_up, w_down):
    dma = pltpu.SemaphoreType.DMA
    bf = jnp.bfloat16
    vm, an = pl.BlockSpec(memory_space=VMEM), pl.BlockSpec(memory_space=ANY)
    chunks = lambda n: VMEM((n, CH_R, CH_C), bf)
    tile = lambda *n: VMEM((*n, *TILE), F32)
    rows, back = VMEM((GRP, CAP_C, MODEL), bf), VMEM((PLN, PITCH, MODEL), bf)
    wide, tall = VMEM((16, 1024), F32), VMEM((512, 128), F32)
    return pl.pallas_call(
        main_kernel,
        out_shape=(jax.ShapeDtypeStruct((64, MODEL), bf), jax.ShapeDtypeStruct((PLN, *TILE), F32)),
        in_specs=[vm, vm, vm, vm, an, an, an],
        out_specs=(vm, vm),
        scratch_shapes=[
            chunks(K), chunks(T), chunks(N_RING), chunks(T),
            VMEM((MODEL, FFN), bf), VMEM((MODEL, FFN), bf), VMEM((FFN, MODEL), bf),
            VMEM((1024, MODEL), bf), rows, rows, rows, rows, back, back, VMEM((512, MODEL), bf), back, back,
            VMEM((GRP * CAP_C, FFN), bf), VMEM((64, MODEL), F32),
            tile(PLN), tile(PLN), tile(PLN), VMEM(TILE, jnp.int32), VMEM((GRP, *TILE), jnp.int32), tile(PLN), tile(2), tile(), tile(2), tile(GRP),
            wide, wide, VMEM((256, 1024), bf), VMEM((256, 1024), bf), VMEM((512, 256), bf), tall, tall,
            VMEM((128, 512), F32), VMEM((128, 512), F32),
            dma((32,)), dma((K // INJ,)), dma((N_SEM,)),
        ],
        compiler_params=pltpu.CompilerParams(collective_id=0, **EFFECTS, vmem_limit_bytes=67043328),
    )(tokens, ids_t, gat_t, counts, w_gate, w_up, w_down)


def sparse_step(tokens, expert_ids, gate_w, route_counts, w_gate, w_up, w_down):
    out, ok_all = main_call(tokens, expert_ids.T, gate_w.T, route_counts, w_gate, w_up, w_down)
    return out, jnp.min(ok_all) > 0.5


def solution(mesh):
    group_size = mesh.shape["ep"]
    row_spec = P(("dp", "ep"))

    def local_step(*args):
        fast, ok = sparse_step(*args)
        return lax.cond(ok, lambda: fast, lambda: dense_step(group_size, *args))

    return jax.shard_map(
        local_step,
        mesh=mesh,
        in_specs=(row_spec, row_spec, row_spec, row_spec, P("ep"), P("ep"), P("ep")),
        out_specs=row_spec,
        check_vma=False,
    )
```
